32 devices in a mesh: data: 8 (over z, y), model: 4 (over x, core).
Axes of the slice: x: 2, y: 2, z: 4, core: 2. Of those that a mesh axis runs over, the one named last changes fastest.
Arguments:
- teacher_in: bfloat16 [32, 3072, 2048], P('data', 'model')
- student_in: bfloat16 [32, 3072, 512], P(('data', 'model'))
- teacher_gain: float32 [1, 2048], replicated
- teacher_up: bfloat16 [1, 2048, 8192], P(None, None, 'model')
- teacher_down: bfloat16 [1, 8192, 2048], P(None, 'model')
- student_gain: float32 [1, 512], replicated
- student_up: bfloat16 [1, 512, 2048], replicated
- student_down: bfloat16 [1, 2048, 512], replicated
- student_proj: bfloat16 [1, 2048, 512], replicated
Outputs:
- output 1: float32 [], replicated
- output 2: float32 [1, 512, 2048], replicated
- output 3: float32 [1, 2048, 512], replicated
- output 4: float32 [1, 512], replicated
- output 5: float32 [1, 2048, 512], replicated
All inputs are finite; a program needn't handle non-finite values.
Results may differ from the reference program's by a relative error of at most 0.00285763.
Values are sent between devices in bfloat16 or wider.
A program may use at most 1 GiB of HBM per device.

```python
import jax
import jax.numpy as jnp
from jax import lax

T_WIDTH = 2048
S_WIDTH = 512
T_LAYERS = 1
N_FEATS = 1
SEQ_LEN = 3072
N_SEQS = 32
EPS = 1e-6


def setup_inputs(seed: int = 0) -> dict:
    keys = jax.random.split(jax.random.key(seed), 9)
    teach_ff = 4 * T_WIDTH
    stud_ff = 4 * S_WIDTH
    base = jax.random.normal(keys[0], (N_SEQS, SEQ_LEN, T_WIDTH), jnp.float32)
    noise = jax.random.normal(keys[1], (N_SEQS, SEQ_LEN, S_WIDTH), jnp.float32)
    return {
        "teacher_in": base.astype(jnp.bfloat16),
        "student_in": (0.8 * base[:, :, :S_WIDTH] + 0.6 * noise).astype(jnp.bfloat16),
        "teacher_gain": jax.random.uniform(keys[2], (T_LAYERS, T_WIDTH), jnp.float32, 0.25, 1.75),
        "teacher_up": (jax.random.normal(keys[3], (T_LAYERS, T_WIDTH, teach_ff), jnp.float32) * T_WIDTH ** -0.5).astype(jnp.bfloat16),
        "teacher_down": (jax.random.normal(keys[4], (T_LAYERS, teach_ff, T_WIDTH), jnp.float32) * teach_ff ** -0.5).astype(jnp.bfloat16),
        "student_gain": jax.random.uniform(keys[5], (N_FEATS, S_WIDTH), jnp.float32, 0.25, 1.75),
        "student_up": (jax.random.normal(keys[6], (N_FEATS, S_WIDTH, stud_ff), jnp.float32) * S_WIDTH ** -0.5).astype(jnp.bfloat16),
        "student_down": (jax.random.normal(keys[7], (N_FEATS, stud_ff, S_WIDTH), jnp.float32) * stud_ff ** -0.5).astype(jnp.bfloat16),
        "student_proj": (jax.random.normal(keys[8], (N_FEATS, T_WIDTH, S_WIDTH), jnp.float32) * T_WIDTH ** -0.5).astype(jnp.bfloat16),
    }


def rms_unit(values):
    return values * lax.rsqrt(jnp.mean(values * values, axis=-1, keepdims=True) + EPS)


def rms_back(values, grad_out):
    inv_rms = lax.rsqrt(jnp.mean(values * values, axis=-1, keepdims=True) + EPS)
    unit = values * inv_rms
    return inv_rms * (grad_out - unit * jnp.mean(grad_out * unit, axis=-1, keepdims=True))


def gelu_back(pre_act, grad_out):
    return jax.vjp(jax.nn.gelu, pre_act)[1](grad_out)[0]


def reference(teacher_in, student_in, teacher_gain, teacher_up, teacher_down, student_gain, student_up, student_down, student_proj):
    t_step = T_LAYERS // N_FEATS
    total = N_FEATS * N_SEQS * SEQ_LEN * S_WIDTH
    grad_scale = 2.0 / total
    teacher_groups = (
        teacher_gain.reshape(N_FEATS, t_step, T_WIDTH),
        teacher_up.reshape(N_FEATS, t_step, T_WIDTH, 4 * T_WIDTH),
        teacher_down.reshape(N_FEATS, t_step, 4 * T_WIDTH, T_WIDTH),
        student_proj,
    )

    def teacher_layer(hidden, layer):
        gain, w_up, w_down = layer
        act_in = (rms_unit(hidden.astype(jnp.float32)) * gain).astype(jnp.bfloat16)
        up_act = jax.nn.gelu(jnp.dot(act_in, w_up, preferred_element_type=jnp.float32)).astype(jnp.bfloat16)
        delta = jnp.dot(up_act, w_down, preferred_element_type=jnp.float32).astype(jnp.bfloat16)
        return (hidden.astype(jnp.float32) + delta.astype(jnp.float32)).astype(jnp.bfloat16), None

    def feature_group(hidden, group):
        gains, ups, downs, project = group
        hidden, _ = lax.scan(teacher_layer, hidden, (gains, ups, downs))
        target = jnp.dot(hidden, project, preferred_element_type=jnp.float32).astype(jnp.bfloat16)
        return hidden, (hidden, target)

    def student_block(state, block):
        gain, w_up, w_down, target = block
        normed = rms_unit(state.astype(jnp.float32))
        act_in = (normed * gain).astype(jnp.bfloat16)
        pre_act = jnp.dot(act_in, w_up, preferred_element_type=jnp.float32)
        up_act = jax.nn.gelu(pre_act).astype(jnp.bfloat16)
        new_state = (state.astype(jnp.float32) + jnp.dot(up_act, w_down, preferred_element_type=jnp.float32)).astype(jnp.bfloat16)
        error = target.astype(jnp.float32) - rms_unit(new_state.astype(jnp.float32))
        return new_state, (state, new_state, error)

    def student_back(d_res, saved):
        state, new_state, error, gain, w_up, w_down = saved
        d_res = d_res + rms_back(new_state.astype(jnp.float32), -grad_scale * error)
        normed = rms_unit(state.astype(jnp.float32))
        act_in = (normed * gain).astype(jnp.bfloat16)
        pre_act = jnp.dot(act_in, w_up, preferred_element_type=jnp.float32)
        up_act = jax.nn.gelu(pre_act).astype(jnp.bfloat16)
        d_out = d_res.astype(jnp.bfloat16)
        g_down = jnp.dot(up_act.T, d_out, preferred_element_type=jnp.float32)
        d_up = jnp.dot(d_out, w_down.T, preferred_element_type=jnp.float32)
        d_pre = gelu_back(pre_act, d_up).astype(jnp.bfloat16)
        g_up = jnp.dot(act_in.T, d_pre, preferred_element_type=jnp.float32)
        d_act = jnp.dot(d_pre, w_up.T, preferred_element_type=jnp.float32)
        g_gain = jnp.sum(d_act * normed, axis=0)
        d_res = d_res + rms_back(state.astype(jnp.float32), d_act * gain)
        return d_res, (g_up, g_down, g_gain)

    def proj_grad(pair):
        feature, error = pair
        return jnp.dot(feature.T, error.astype(jnp.bfloat16), preferred_element_type=jnp.float32)

    def one_sequence(carry, rows):
        teach_row, stud_row = rows
        _, (features, targets) = lax.scan(feature_group, teach_row, teacher_groups)
        _, saved = lax.scan(student_block, stud_row, (student_gain, student_up, student_down, targets))
        states, new_states, errors = saved
        _, (g_up, g_down, g_gain) = lax.scan(
            student_back,
            jnp.zeros((SEQ_LEN, S_WIDTH), jnp.float32),
            (states, new_states, errors, student_gain, student_up, student_down),
            reverse=True,
        )
        g_proj = grad_scale * lax.map(proj_grad, (features, errors))
        increment = (jnp.sum(errors * errors), g_up, g_down, g_gain, g_proj)
        return jax.tree.map(jnp.add, carry, increment), None

    start_sums = (
        jnp.zeros((), jnp.float32),
        jnp.zeros((N_FEATS, S_WIDTH, 4 * S_WIDTH), jnp.float32),
        jnp.zeros((N_FEATS, 4 * S_WIDTH, S_WIDTH), jnp.float32),
        jnp.zeros((N_FEATS, S_WIDTH), jnp.float32),
        jnp.zeros((N_FEATS, T_WIDTH, S_WIDTH), jnp.float32),
    )
    totals, _ = lax.scan(one_sequence, start_sums, (teacher_in, student_in))
    return (totals[0] / total, totals[1], totals[2], totals[3], totals[4])
```

```python
import jax
import jax.numpy as jnp
from jax import lax
from jax.experimental import pallas as pl
from jax.experimental.pallas import tpu as pltpu
from jax.sharding import PartitionSpec as P

EPS = 1e-6
MESH = pl.DeviceIdType.MESH
F32 = jnp.float32
BF16 = jnp.bfloat16
GELU_K = 0.7978845608028654
GELU_C = 0.044715
TILE = 512
CHUNK = 512
PIECES = 8
X_STEPS = (10, 20, 30, 40, 50, 60, 66, 70)
VMEM_LIMIT = 67043328


def gelu(x):
    return 0.5 * x * (1.0 + jnp.tanh(GELU_K * (x + GELU_C * (x * x * x))))


def teacher_kernel(
    h_ref, gain_ref, w1_ref, w2_ref, s_ref,
    f_ref, w1g, w2g, sx_ref,
    act, acc, w1_v, w2_v, u_a, u_b, s_v,
    x_send, x_recv, y_send, y_recv, d_send, d_recv, g_send, g_recv, s_send, s_recv,
    w_sem, h_sem, f_sem, s_sem,
):
    data = lax.axis_index("data")
    model = lax.axis_index("model")
    y_par = lax.rem(data, 2)
    sib = (data, model + 1 - 2 * lax.rem(model, 2))
    x_nbr = (data, lax.rem(model + 2, 4))
    y_nbr = (data + 1 - 2 * y_par, model)
    rows, width = act.shape
    quarter = w1_ref.shape[1]
    half = quarter // 2
    piece = half // PIECES
    n_tiles = rows // TILE
    per_quarter = quarter // CHUNK
    n_chunks = 4 * per_quarter
    half_chunks = half // CHUNK
    per_chunk = CHUNK // piece

    def remote(src1, dst1, src2, dst2, send, recv, target):
        return (
            pltpu.make_async_remote_copy(src_ref=src1, dst_ref=dst1, send_sem=send.at[0], recv_sem=recv.at[0], device_id=target, device_id_type=MESH),
            pltpu.make_async_remote_copy(src_ref=src2, dst_ref=dst2, send_sem=send.at[1], recv_sem=recv.at[1], device_id=target, device_id_type=MESH),
        )

    def cols(start, size):
        return pl.ds(pl.multiple_of(start, size), size)

    def x_copy(p):
        where = cols(y_par * half + p * piece, piece)
        return remote(w1_ref.at[:, where], w1g.at[1, :, where], w2_ref.at[where], w2g.at[1, where], x_send.at[p], x_recv.at[p], x_nbr)

    def y_copy(p, mine):
        where = cols((y_par if mine else 1 - y_par) * half + p * piece, piece)
        return remote(w1g.at[1, :, where], w1g.at[1, :, where], w2g.at[1, where], w2g.at[1, where], y_send.at[p], y_recv.at[p], y_nbr)

    def d_copy(i):
        where = cols(i * CHUNK, CHUNK)
        return remote(w1_ref.at[:, where], w1g.at[0, :, where], w2_ref.at[where], w2g.at[0, where], d_send.at[i], d_recv.at[i], sib)

    def far_cols(group):
        side = y_par if group % 2 == 0 else 1 - y_par
        return cols(side * half + (group // 2) * CHUNK, CHUNK)

    def g_copy(group):
        where = far_cols(group)
        return remote(w1g.at[1, :, where], w1g.at[2, :, where], w2g.at[1, where], w2g.at[2, where], g_send.at[group], g_recv.at[group], sib)

    def s_copy(k):
        other = lax.rem(model + k, 4)
        return pltpu.make_async_remote_copy(
            src_ref=s_ref.at[other], dst_ref=sx_ref.at[model], send_sem=s_send.at[k - 1], recv_sem=s_recv.at[k - 1],
            device_id=(data, other), device_id_type=MESH,
        )

    def s_arrival(k):
        other = lax.rem(model + 4 - k, 4)
        return pltpu.make_async_remote_copy(
            src_ref=s_ref.at[other], dst_ref=sx_ref.at[other], send_sem=s_send.at[k - 1], recv_sem=s_recv.at[k - 1],
            device_id=(data, other), device_id_type=MESH,
        )

    def load(src1, src2, slot):
        pltpu.make_async_copy(src1, w1_v.at[slot], w_sem.at[slot, 0]).start()
        pltpu.make_async_copy(src2, w2_v.at[slot], w_sem.at[slot, 1]).start()

    def load_wait(slot):
        pltpu.make_async_copy(w1_ref.at[:, pl.ds(0, CHUNK)], w1_v.at[slot], w_sem.at[slot, 0]).wait()
        pltpu.make_async_copy(w2_ref.at[pl.ds(0, CHUNK)], w2_v.at[slot], w_sem.at[slot, 1]).wait()

    def tile_rows(t):
        return pl.ds(pl.multiple_of(t * TILE, TILE), TILE)

    def h_load(t):
        return pltpu.make_async_copy(h_ref.at[tile_rows(t)], act.at[tile_rows(t)], h_sem.at[t])

    def f_store(t):
        return pltpu.make_async_copy(act.at[tile_rows(t)], f_ref.at[tile_rows(t)], f_sem.at[t])

    for t in range(n_tiles):
        h_load(t).start()
    load(w1_ref.at[:, pl.ds(0, CHUNK)], w2_ref.at[pl.ds(0, CHUNK)], 0)
    own_in = pltpu.make_async_copy(s_ref.at[model], s_v, s_sem.at[0])
    own_in.start()

    barrier = pltpu.get_barrier_semaphore()
    others = [(data, lax.rem(model + k, 4)) for k in (1, 2, 3)] + [y_nbr]
    for other in others:
        pl.semaphore_signal(barrier, inc=1, device_id=other, device_id_type=MESH)
    pl.semaphore_wait(barrier, len(others))

    for p in range(2):
        for copy in x_copy(p):
            copy.start()
    for i in range(per_quarter):
        for copy in d_copy(i):
            copy.start()

    u_b[...] = jnp.zeros_like(u_b)
    sub = 32

    @pl.loop(0, n_tiles)
    def _(t):
        h_load(t).wait()

        @pl.loop(0, TILE // sub)
        def _(k):
            where = pl.ds(pl.multiple_of(t * TILE + k * sub, sub), sub)
            values = act[where, :].astype(F32)
            inv = lax.rsqrt(jnp.mean(values * values, axis=-1, keepdims=True) + EPS)
            act[where, :] = ((values * inv) * gain_ref[...]).astype(BF16)
            acc[where, :] = jnp.zeros((sub, width), F32)

    own_in.wait()
    own_out = pltpu.make_async_copy(s_v, sx_ref.at[model], s_sem.at[1])
    own_out.start()

    pairs = n_tiles // 2

    @pl.loop(0, n_chunks * pairs)
    def _(i):
        c = i // pairs
        j = lax.rem(i, pairs)
        slot = lax.rem(c, 2)
        first = 2 * j
        before = lax.rem(first + n_tiles - 1, n_tiles)
        slot_before = jnp.where((j == 0) & (c > 0), 1 - slot, slot)

        for p, step in enumerate(X_STEPS):

            @pl.when(2 * i == step)
            def _(p=p):
                for copy in x_copy(p):
                    copy.wait_recv()
                for copy in y_copy(p, True):
                    copy.start()
                if p + 2 < PIECES:
                    for copy in x_copy(p + 2):
                        copy.start()
                if p == PIECES - 2:
                    for k in (1, 2, 3):
                        s_copy(k).start()
                if p % per_chunk == per_chunk - 1:
                    for copy in g_copy(2 * (p // per_chunk)):
                        copy.start()

        @pl.when((j == 0))
        def _():
            load_wait(slot)

        coming = c + 1
        loads = j == pairs - 1

        @pl.when(loads & (coming < per_quarter))
        def _():
            where = cols(coming * CHUNK, CHUNK)
            load(w1_ref.at[:, where], w2_ref.at[where], 1 - slot)

        for k in range(per_quarter):

            @pl.when(loads & (coming == per_quarter + k))
            def _(k=k):
                for copy in d_copy(k):
                    copy.wait_recv()
                where = cols(k * CHUNK, CHUNK)
                load(w1g.at[0, :, where], w2g.at[0, where], 1 - slot)

        for group in range(per_quarter):
            place = 2 * per_quarter + 2 * group

            @pl.when(loads & (coming == place))
            def _(group=group):
                if group % 2 == 1:
                    for q in range(per_chunk):
                        for copy in y_copy((group // 2) * per_chunk + q, False):
                            copy.wait_recv()
                    for copy in g_copy(group):
                        copy.start()
                where = far_cols(group)
                load(w1g.at[1, :, where], w2g.at[1, where], 1 - slot)

            @pl.when(loads & (coming == place + 1))
            def _(group=group):
                for copy in g_copy(group):
                    copy.wait_recv()
                where = far_cols(group)
                load(w1g.at[2, :, where], w2g.at[2, where], 1 - slot)

        @pl.when((c == n_chunks - 1) & (j > 0))
        def _():
            h_load(first - 2).start()
            h_load(first - 1).start()

        u_a[...] = gelu(jnp.dot(act[tile_rows(first), :], w1_v[slot], preferred_element_type=F32)).astype(BF16)
        acc[tile_rows(before), :] += jnp.dot(u_b[...], w2_v[slot_before], preferred_element_type=F32)
        u_b[...] = gelu(jnp.dot(act[tile_rows(first + 1), :], w1_v[slot], preferred_element_type=F32)).astype(BF16)
        acc[tile_rows(first), :] += jnp.dot(u_a[...], w2_v[slot], preferred_element_type=F32)

    h_load(n_tiles - 2).start()
    h_load(n_tiles - 1).start()
    acc[pl.ds((n_tiles - 1) * TILE, TILE), :] += jnp.dot(u_b[...], w2_v[(n_chunks - 1) % 2], preferred_element_type=F32)

    @pl.loop(0, n_tiles)
    def _(t):
        h_load(t).wait()

        @pl.loop(0, TILE // sub)
        def _(k):
            where = pl.ds(pl.multiple_of(t * TILE + k * sub, sub), sub)
            delta = acc[where, :].astype(BF16).astype(F32)
            act[where, :] = (act[where, :].astype(F32) + delta).astype(BF16)

        f_store(t).start()

    for k in (1, 2, 3):
        s_arrival(k).wait_recv()
        s_copy(k).wait_send()
    own_out.wait()
    for p in range(PIECES):
        for copy in x_copy(p) + y_copy(p, True):
            copy.wait_send()
    for i in range(per_quarter):
        for copy in d_copy(i) + g_copy(i):
            copy.wait_send()
    for t in range(n_tiles):
        f_store(t).wait()


def teacher_layer(hidden, gain, w_up, w_down, student_rows):
    rows, width = hidden.shape
    quarter = w_up.shape[1]
    per_quarter = quarter // CHUNK
    n_tiles = rows // TILE
    dma = pltpu.SemaphoreType.DMA
    anywhere = pl.BlockSpec(memory_space=pl.ANY)
    return pl.pallas_call(
        teacher_kernel,
        out_shape=(
            jax.ShapeDtypeStruct((rows, width), BF16),
            jax.ShapeDtypeStruct((3, width, quarter), BF16),
            jax.ShapeDtypeStruct((3, quarter, width), BF16),
            jax.ShapeDtypeStruct(student_rows.shape, BF16),
        ),
        in_specs=[anywhere, pl.BlockSpec(memory_space=pltpu.VMEM), anywhere, anywhere, anywhere],
        out_specs=(anywhere,) * 4,
        scratch_shapes=[
            pltpu.VMEM((rows, width), BF16),
            pltpu.VMEM((rows, width), F32),
            pltpu.VMEM((2, width, CHUNK), BF16),
            pltpu.VMEM((2, CHUNK, width), BF16),
            pltpu.VMEM((TILE, CHUNK), BF16),
            pltpu.VMEM((TILE, CHUNK), BF16),
            pltpu.VMEM(student_rows.shape[1:], BF16),
            dma((PIECES, 2)), dma((PIECES, 2)), dma((PIECES, 2)), dma((PIECES, 2)),
            dma((per_quarter, 2)), dma((per_quarter, 2)), dma((per_quarter, 2)), dma((per_quarter, 2)),
            dma((3,)), dma((3,)),
            dma((2, 2)), dma((n_tiles,)), dma((n_tiles,)), dma((2,)),
        ],
        compiler_params=pltpu.CompilerParams(collective_id=0, has_side_effects=True, vmem_limit_bytes=VMEM_LIMIT),
        cost_estimate=pl.CostEstimate(flops=16 * rows * width * quarter, bytes_accessed=8 * width * quarter * 2, transcendentals=0),
        name="teacher",
    )(hidden, gain, w_up, w_down, student_rows)


def nt_dot(a, b):
    return lax.dot_general(a, b, (((1,), (1,)), ((), ())), preferred_element_type=F32)


def tn_dot(a, b):
    return lax.dot_general(a, b, (((0,), (0,)), ((), ())), preferred_element_type=F32)


def student_kernel(scale_ref, f_ref, s_ref, gain_ref, up_ref, down_ref, proj_ref, g_ref, pre, err_t):
    i = pl.program_id(0)
    width = s_ref.shape[1]
    scale = scale_ref[0]

    @pl.when(i == 0)
    def _():
        g_ref[...] = jnp.zeros_like(g_ref)

    state = s_ref[...].astype(F32)
    normed = state * lax.rsqrt(jnp.mean(state * state, axis=-1, keepdims=True) + EPS)
    act_in = (normed * gain_ref[...]).astype(BF16)
    pre[...] = jnp.dot(act_in, up_ref[...], preferred_element_type=F32)
    up_act = gelu(pre[...]).astype(BF16)
    new_state = (state + jnp.dot(up_act, down_ref[...], preferred_element_type=F32)).astype(BF16).astype(F32)
    target = jnp.dot(f_ref[...], proj_ref[...], preferred_element_type=F32).astype(BF16).astype(F32)
    inv = lax.rsqrt(jnp.mean(new_state * new_state, axis=-1, keepdims=True) + EPS)
    unit = new_state * inv
    error = target - unit
    grad = -scale * error
    d_res = inv * (grad - unit * jnp.mean(grad * unit, axis=-1, keepdims=True))
    d_out = d_res.astype(BF16)
    g_ref[pl.ds(2 * width, width), :] += scale * tn_dot(error.astype(BF16), f_ref[...])
    g_ref[pl.ds(width, width), :] += tn_dot(d_out, up_act)
    d_up = nt_dot(d_out, down_ref[...])
    x = pre[...]
    x2 = x * x
    th = jnp.tanh(GELU_K * (x + GELU_C * (x2 * x)))
    slope = 0.5 * (1.0 + th) + 0.5 * x * (1.0 - th * th) * (GELU_K * (1.0 + 3.0 * GELU_C * x2))
    d_pre = (slope * d_up).astype(BF16)
    g_ref[pl.ds(0, width), :] += tn_dot(act_in, d_pre)
    d_act = nt_dot(d_pre, up_ref[...])
    g_ref[pl.ds(3 * width, 1), pl.ds(0, width)] += jnp.sum(d_act * normed, axis=0, keepdims=True)
    squares = jnp.sum(error * error, axis=0, keepdims=True)
    g_ref[pl.ds(3 * width, 1), pl.ds(width, width)] += squares


def student_layer(scale, feature, student_rows, gain, w_up, w_down, proj):
    rows, t_width = feature.shape
    width = student_rows.shape[1]
    wide = w_up.shape[1]
    tile = 512
    whole = pl.BlockSpec(memory_space=pltpu.VMEM)
    return pl.pallas_call(
        student_kernel,
        out_shape=jax.ShapeDtypeStruct((3 * width + 8, wide), F32),
        grid=(rows // tile,),
        in_specs=[
            pl.BlockSpec(memory_space=pltpu.SMEM),
            pl.BlockSpec((tile, t_width), lambda i: (i, 0)),
            pl.BlockSpec((tile, width), lambda i: (i, 0)),
            whole, whole, whole, whole,
        ],
        out_specs=pl.BlockSpec(memory_space=pltpu.VMEM),
        scratch_shapes=[pltpu.VMEM((tile, wide), F32), pltpu.VMEM((8, 128), F32)],
        compiler_params=pltpu.CompilerParams(dimension_semantics=("arbitrary",), vmem_limit_bytes=VMEM_LIMIT),
        cost_estimate=pl.CostEstimate(flops=12 * rows * width * wide + 4 * rows * width * t_width, bytes_accessed=2 * rows * (t_width + width), transcendentals=0),
        name="student",
    )(scale, feature, student_rows, gain, w_up, w_down, proj)


def solution(mesh):
    dev_count = mesh.shape["data"] * mesh.shape["model"]
    all_axes = ("data", "model")

    def body(teacher_in, student_in, teacher_gain, teacher_up, teacher_down, student_gain, student_up, student_down, student_proj):
        seqs, tokens, t_width = teacher_in.shape
        seq_rows, seq_len, width = student_in.shape
        total = seq_rows * dev_count * seq_len * width
        grad_scale = 2.0 / total
        feature, _, _, rows = teacher_layer(
            teacher_in.reshape(seqs * tokens, t_width), teacher_gain, teacher_up[0], teacher_down[0],
            student_in.reshape(seqs, tokens, width),
        )
        sums = student_layer(
            jnp.full((1,), grad_scale, F32), feature, rows.reshape(seqs * tokens, width),
            student_gain, student_up[0], student_down[0], student_proj[0],
        )
        sums = lax.psum(sums, all_axes)
        grad_up = sums[None, :width]
        grad_down = sums[width : 2 * width].T[None]
        grad_proj = sums[2 * width : 3 * width].T[None]
        grad_gain = sums[None, 3 * width, :width]
        loss = jnp.sum(sums[3 * width, width : 2 * width]) / total
        return (loss, grad_up, grad_down, grad_gain, grad_proj)

    return jax.shard_map(
        body,
        mesh=mesh,
        in_specs=(
            P("data", "model", None),
            P(("data", "model"), None, None),
            P(),
            P(None, None, "model"),
            P(None, "model", None),
            P(),
            P(),
            P(),
            P(),
        ),
        out_specs=(P(), P(), P(), P(), P()),
        check_vma=False,
    )
```

```python
import jax
import jax.numpy as jnp
from jax import lax
from jax.experimental import pallas as pl
from jax.experimental.pallas import tpu as pltpu
from jax.sharding import PartitionSpec as P

EPS = 1e-6
MESH = pl.DeviceIdType.MESH
F32 = jnp.float32
BF16 = jnp.bfloat16
GELU_K = 0.7978845608028654
GELU_C = 0.044715
TILE = 512
CHUNK = 512
PIECES = 8
X_STEPS = (10, 20, 30, 40, 50, 60, 66, 70)
VMEM_LIMIT = 67043328


def gelu(x):
    return 0.5 * x * (1.0 + jnp.tanh(GELU_K * (x + GELU_C * (x * x * x))))


def teacher_kernel(
    h_ref, gain_ref, w1_ref, w2_ref, s_ref,
    f_ref, w1g, w2g, sx_ref,
    act, acc, w1_v, w2_v, u_a, u_b, s_v,
    x_send, x_recv, y_send, y_recv, d_send, d_recv, g_send, g_recv, s_send, s_recv,
    w_sem, h_sem, f_sem, s_sem,
):
    data = lax.axis_index("data")
    model = lax.axis_index("model")
    y_par = lax.rem(data, 2)
    sib = (data, model + 1 - 2 * lax.rem(model, 2))
    x_nbr = (data, lax.rem(model + 2, 4))
    y_nbr = (data + 1 - 2 * y_par, model)
    rows, width = act.shape
    quarter = w1_ref.shape[1]
    half = quarter // 2
    piece = half // PIECES
    n_tiles = rows // TILE
    per_quarter = quarter // CHUNK
    n_chunks = 4 * per_quarter
    half_chunks = half // CHUNK
    per_chunk = CHUNK // piece

    def remote(src1, dst1, src2, dst2, send, recv, target):
        return (
            pltpu.make_async_remote_copy(src_ref=src1, dst_ref=dst1, send_sem=send.at[0], recv_sem=recv.at[0], device_id=target, device_id_type=MESH),
            pltpu.make_async_remote_copy(src_ref=src2, dst_ref=dst2, send_sem=send.at[1], recv_sem=recv.at[1], device_id=target, device_id_type=MESH),
        )

    def cols(start, size):
        return pl.ds(pl.multiple_of(start, size), size)

    def x_copy(p):
        where = cols(y_par * half + p * piece, piece)
        return remote(w1_ref.at[:, where], w1g.at[1, :, where], w2_ref.at[where], w2g.at[1, where], x_send.at[p], x_recv.at[p], x_nbr)

    def y_copy(p, mine):
        where = cols((y_par if mine else 1 - y_par) * half + p * piece, piece)
        return remote(w1g.at[1, :, where], w1g.at[1, :, where], w2g.at[1, where], w2g.at[1, where], y_send.at[p], y_recv.at[p], y_nbr)

    def d_copy(i):
        where = cols(i * CHUNK, CHUNK)
        return remote(w1_ref.at[:, where], w1g.at[0, :, where], w2_ref.at[where], w2g.at[0, where], d_send.at[i], d_recv.at[i], sib)

    def far_cols(group):
        side = y_par if group % 2 == 0 else 1 - y_par
        return cols(side * half + (group // 2) * CHUNK, CHUNK)

    def g_copy(group):
        where = far_cols(group)
        return remote(w1g.at[1, :, where], w1g.at[2, :, where], w2g.at[1, where], w2g.at[2, where], g_send.at[group], g_recv.at[group], sib)

    def s_copy(k):
        other = lax.rem(model + k, 4)
        return pltpu.make_async_remote_copy(
            src_ref=s_ref.at[other], dst_ref=sx_ref.at[model], send_sem=s_send.at[k - 1], recv_sem=s_recv.at[k - 1],
            device_id=(data, other), device_id_type=MESH,
        )

    def s_arrival(k):
        other = lax.rem(model + 4 - k, 4)
        return pltpu.make_async_remote_copy(
            src_ref=s_ref.at[other], dst_ref=sx_ref.at[other], send_sem=s_send.at[k - 1], recv_sem=s_recv.at[k - 1],
            device_id=(data, other), device_id_type=MESH,
        )

    def load(src1, src2, slot):
        pltpu.make_async_copy(src1, w1_v.at[slot], w_sem.at[slot, 0]).start()
        pltpu.make_async_copy(src2, w2_v.at[slot], w_sem.at[slot, 1]).start()

    def load_wait(slot):
        pltpu.make_async_copy(w1_ref.at[:, pl.ds(0, CHUNK)], w1_v.at[slot], w_sem.at[slot, 0]).wait()
        pltpu.make_async_copy(w2_ref.at[pl.ds(0, CHUNK)], w2_v.at[slot], w_sem.at[slot, 1]).wait()

    def tile_rows(t):
        return pl.ds(pl.multiple_of(t * TILE, TILE), TILE)

    def h_load(t):
        return pltpu.make_async_copy(h_ref.at[tile_rows(t)], act.at[tile_rows(t)], h_sem.at[t])

    def f_store(t):
        return pltpu.make_async_copy(act.at[tile_rows(t)], f_ref.at[tile_rows(t)], f_sem.at[t])

    for t in range(n_tiles):
        h_load(t).start()
    load(w1_ref.at[:, pl.ds(0, CHUNK)], w2_ref.at[pl.ds(0, CHUNK)], 0)
    own_in = pltpu.make_async_copy(s_ref.at[model], s_v, s_sem.at[0])
    own_in.start()

    barrier = pltpu.get_barrier_semaphore()
    others = [(data, lax.rem(model + k, 4)) for k in (1, 2, 3)] + [y_nbr]
    for other in others:
        pl.semaphore_signal(barrier, inc=1, device_id=other, device_id_type=MESH)
    pl.semaphore_wait(barrier, len(others))

    for p in range(2):
        for copy in x_copy(p):
            copy.start()
    for i in range(per_quarter):
        for copy in d_copy(i):
            copy.start()

    u_b[...] = jnp.zeros_like(u_b)
    sub = 32

    @pl.loop(0, n_tiles)
    def _(t):
        h_load(t).wait()

        @pl.loop(0, TILE // sub)
        def _(k):
            where = pl.ds(pl.multiple_of(t * TILE + k * sub, sub), sub)
            values = act[where, :].astype(F32)
            inv = lax.rsqrt(jnp.mean(values * values, axis=-1, keepdims=True) + EPS)
            act[where, :] = ((values * inv) * gain_ref[...]).astype(BF16)
            acc[where, :] = jnp.zeros((sub, width), F32)

    own_in.wait()
    own_out = pltpu.make_async_copy(s_v, sx_ref.at[model], s_sem.at[1])
    own_out.start()

    pairs = n_tiles // 2

    @pl.loop(0, n_chunks * pairs)
    def _(i):
        c = i // pairs
        j = lax.rem(i, pairs)
        slot = lax.rem(c, 2)
        first = 2 * j
        before = lax.rem(first + n_tiles - 1, n_tiles)
        slot_before = jnp.where((j == 0) & (c > 0), 1 - slot, slot)

        for p, step in enumerate(X_STEPS):

            @pl.when(2 * i == step)
            def _(p=p):
                for copy in x_copy(p):
                    copy.wait_recv()
                for copy in y_copy(p, True):
                    copy.start()
                if p + 2 < PIECES:
                    for copy in x_copy(p + 2):
                        copy.start()
                if p == PIECES - 2:
                    for k in (1, 2, 3):
                        s_copy(k).start()
                if p % per_chunk == per_chunk - 1:
                    for copy in g_copy(2 * (p // per_chunk)):
                        copy.start()

        @pl.when((j == 0))
        def _():
            load_wait(slot)

        coming = c + 1
        loads = j == pairs - 1

        @pl.when(loads & (coming < per_quarter))
        def _():
            where = cols(coming * CHUNK, CHUNK)
            load(w1_ref.at[:, where], w2_ref.at[where], 1 - slot)

        for k in range(per_quarter):

            @pl.when(loads & (coming == per_quarter + k))
            def _(k=k):
                for copy in d_copy(k):
                    copy.wait_recv()
                where = cols(k * CHUNK, CHUNK)
                load(w1g.at[0, :, where], w2g.at[0, where], 1 - slot)

        for group in range(per_quarter):
            place = 2 * per_quarter + 2 * group

            @pl.when(loads & (coming == place))
            def _(group=group):
                if group % 2 == 1:
                    for q in range(per_chunk):
                        for copy in y_copy((group // 2) * per_chunk + q, False):
                            copy.wait_recv()
                    for copy in g_copy(group):
                        copy.start()
                where = far_cols(group)
                load(w1g.at[1, :, where], w2g.at[1, where], 1 - slot)

            @pl.when(loads & (coming == place + 1))
            def _(group=group):
                for copy in g_copy(group):
                    copy.wait_recv()
                where = far_cols(group)
                load(w1g.at[2, :, where], w2g.at[2, where], 1 - slot)

        @pl.when((c == n_chunks - 1) & (j > 0))
        def _():
            h_load(first - 2).start()
            h_load(first - 1).start()

        u_a[...] = gelu(jnp.dot(act[tile_rows(first), :], w1_v[slot], preferred_element_type=F32)).astype(BF16)
        acc[tile_rows(before), :] += jnp.dot(u_b[...], w2_v[slot_before], preferred_element_type=F32)
        u_b[...] = gelu(jnp.dot(act[tile_rows(first + 1), :], w1_v[slot], preferred_element_type=F32)).astype(BF16)
        acc[tile_rows(first), :] += jnp.dot(u_a[...], w2_v[slot], preferred_element_type=F32)

    h_load(n_tiles - 2).start()
    h_load(n_tiles - 1).start()
    acc[pl.ds((n_tiles - 1) * TILE, TILE), :] += jnp.dot(u_b[...], w2_v[(n_chunks - 1) % 2], preferred_element_type=F32)

    @pl.loop(0, n_tiles)
    def _(t):
        h_load(t).wait()

        @pl.loop(0, TILE // sub)
        def _(k):
            where = pl.ds(pl.multiple_of(t * TILE + k * sub, sub), sub)
            delta = acc[where, :].astype(BF16).astype(F32)
            act[where, :] = (act[where, :].astype(F32) + delta).astype(BF16)

        f_store(t).start()

    for k in (1, 2, 3):
        s_arrival(k).wait_recv()
        s_copy(k).wait_send()
    own_out.wait()
    for p in range(PIECES):
        for copy in x_copy(p) + y_copy(p, True):
            copy.wait_send()
    for i in range(per_quarter):
        for copy in d_copy(i) + g_copy(i):
            copy.wait_send()
    for t in range(n_tiles):
        f_store(t).wait()


def teacher_layer(hidden, gain, w_up, w_down, student_rows):
    rows, width = hidden.shape
    quarter = w_up.shape[1]
    per_quarter = quarter // CHUNK
    n_tiles = rows // TILE
    dma = pltpu.SemaphoreType.DMA
    anywhere = pl.BlockSpec(memory_space=pl.ANY)
    return pl.pallas_call(
        teacher_kernel,
        out_shape=(
            jax.ShapeDtypeStruct((rows, width), BF16),
            jax.ShapeDtypeStruct((3, width, quarter), BF16),
            jax.ShapeDtypeStruct((3, quarter, width), BF16),
            jax.ShapeDtypeStruct(student_rows.shape, BF16),
        ),
        in_specs=[anywhere, pl.BlockSpec(memory_space=pltpu.VMEM), anywhere, anywhere, anywhere],
        out_specs=(anywhere,) * 4,
        scratch_shapes=[
            pltpu.VMEM((rows, width), BF16),
            pltpu.VMEM((rows, width), F32),
            pltpu.VMEM((2, width, CHUNK), BF16),
            pltpu.VMEM((2, CHUNK, width), BF16),
            pltpu.VMEM((TILE, CHUNK), BF16),
            pltpu.VMEM((TILE, CHUNK), BF16),
            pltpu.VMEM(student_rows.shape[1:], BF16),
            dma((PIECES, 2)), dma((PIECES, 2)), dma((PIECES, 2)), dma((PIECES, 2)),
            dma((per_quarter, 2)), dma((per_quarter, 2)), dma((per_quarter, 2)), dma((per_quarter, 2)),
            dma((3,)), dma((3,)),
            dma((2, 2)), dma((n_tiles,)), dma((n_tiles,)), dma((2,)),
        ],
        compiler_params=pltpu.CompilerParams(collective_id=0, has_side_effects=True, vmem_limit_bytes=VMEM_LIMIT),
        cost_estimate=pl.CostEstimate(flops=16 * rows * width * quarter, bytes_accessed=8 * width * quarter * 2, transcendentals=0),
        name="teacher",
    )(hidden, gain, w_up, w_down, student_rows)


def nt_dot(a, b):
    return lax.dot_general(a, b, (((1,), (1,)), ((), ())), preferred_element_type=F32)


def tn_dot(a, b):
    return lax.dot_general(a, b, (((0,), (0,)), ((), ())), preferred_element_type=F32)


def student_kernel(scale_ref, f_ref, s_ref, gain_ref, up_ref, down_ref, proj_ref, g_ref, small_ref, pre):
    i = pl.program_id(0)
    width = s_ref.shape[1]
    scale = scale_ref[0]

    @pl.when(i == 0)
    def _():
        g_ref[...] = jnp.zeros_like(g_ref)
        small_ref[...] = jnp.zeros_like(small_ref)

    state = s_ref[...].astype(F32)
    normed = state * lax.rsqrt(jnp.mean(state * state, axis=-1, keepdims=True) + EPS)
    act_in = (normed * gain_ref[...]).astype(BF16)
    pre[...] = jnp.dot(act_in, up_ref[...], preferred_element_type=F32)
    up_act = gelu(pre[...]).astype(BF16)
    new_state = (state + jnp.dot(up_act, down_ref[...], preferred_element_type=F32)).astype(BF16).astype(F32)
    target = jnp.dot(f_ref[...], proj_ref[...], preferred_element_type=F32).astype(BF16).astype(F32)
    inv = lax.rsqrt(jnp.mean(new_state * new_state, axis=-1, keepdims=True) + EPS)
    unit = new_state * inv
    error = target - unit
    grad = -scale * error
    d_res = inv * (grad - unit * jnp.mean(grad * unit, axis=-1, keepdims=True))
    d_out = d_res.astype(BF16)
    g_ref[pl.ds(2 * width, width), :] += scale * tn_dot(error.astype(BF16), f_ref[...])
    g_ref[pl.ds(width, width), :] += tn_dot(d_out, up_act)
    d_up = nt_dot(d_out, down_ref[...])
    x = pre[...]
    x2 = x * x
    th = jnp.tanh(GELU_K * (x + GELU_C * (x2 * x)))
    slope = 0.5 * (1.0 + th) + 0.5 * x * (1.0 - th * th) * (GELU_K * (1.0 + 3.0 * GELU_C * x2))
    d_pre = (slope * d_up).astype(BF16)
    g_ref[pl.ds(0, width), :] += tn_dot(act_in, d_pre)
    d_act = nt_dot(d_pre, up_ref[...])
    small_ref[pl.ds(0, 1), :] += jnp.sum(d_act * normed, axis=0, keepdims=True)
    squares = jnp.sum(error * error, axis=0, keepdims=True)
    small_ref[pl.ds(1, 1), :] += squares


def student_layer(scale, feature, student_rows, gain, w_up, w_down, proj):
    rows, t_width = feature.shape
    width = student_rows.shape[1]
    wide = w_up.shape[1]
    tile = 512
    whole = pl.BlockSpec(memory_space=pltpu.VMEM)
    return pl.pallas_call(
        student_kernel,
        out_shape=(jax.ShapeDtypeStruct((3 * width, wide), F32), jax.ShapeDtypeStruct((8, width), F32)),
        grid=(rows // tile,),
        in_specs=[
            pl.BlockSpec(memory_space=pltpu.SMEM),
            pl.BlockSpec((tile, t_width), lambda i: (i, 0)),
            pl.BlockSpec((tile, width), lambda i: (i, 0)),
            whole, whole, whole, whole,
        ],
        out_specs=(pl.BlockSpec(memory_space=pltpu.VMEM),) * 2,
        scratch_shapes=[pltpu.VMEM((tile, wide), F32)],
        compiler_params=pltpu.CompilerParams(dimension_semantics=("arbitrary",), vmem_limit_bytes=VMEM_LIMIT),
        cost_estimate=pl.CostEstimate(flops=12 * rows * width * wide + 4 * rows * width * t_width, bytes_accessed=2 * rows * (t_width + width), transcendentals=0),
        name="student",
    )(scale, feature, student_rows, gain, w_up, w_down, proj)


def total_kernel(
    g_ref, small_ref, out_ref, small_out,
    work, inbox, whole, small_v, small_in,
    rs_send, rs_recv, ag_send, ag_recv, sm_send, sm_recv, in_sem, out_sem,
):
    data = lax.axis_index("data")
    model = lax.axis_index("model")
    bits = {
        "core": lax.rem(model, 2),
        "x": model // 2,
        "y": lax.rem(data, 2),
        "z": lax.rem(data // 2, 2),
        "zz": data // 4,
    }
    turn = {name: 1 - 2 * bit for name, bit in bits.items()}
    partner = {
        "core": (data, model + turn["core"]),
        "x": (data, model + 2 * turn["x"]),
        "y": (data + turn["y"], model),
        "z": (data + 2 * turn["z"], model),
        "zz": (data + 4 * turn["zz"], model),
    }
    orders = (("core", "x", "y", "z", "zz"), ("core", "y", "z", "x", "zz"), ("core", "z", "x", "y", "zz"))
    stages = len(orders[0])
    parts = len(orders)
    height = work.shape[0] // parts
    sizes = [height >> (k + 1) for k in range(stages)]
    slots = [height - (height >> k) for k in range(stages)]

    def block(start, size):
        return pl.ds(pl.multiple_of(start, size), size)

    for part in range(parts):
        pltpu.make_async_copy(g_ref.at[pl.ds(part * height, height)], work.at[pl.ds(part * height, height)], in_sem.at[part]).start()

    barrier = pltpu.get_barrier_semaphore()
    for target in partner.values():
        pl.semaphore_signal(barrier, inc=1, device_id=target, device_id_type=MESH)
    pl.semaphore_wait(barrier, stages)

    bases = [[part * height] for part in range(parts)]
    for part in range(parts):
        for k in range(stages):
            bases[part].append(bases[part][k] + bits[orders[part][k]] * sizes[k])

    def rs_copy(part, k):
        name = orders[part][k]
        gone = block(bases[part][k] + (1 - bits[name]) * sizes[k], sizes[k])
        return pltpu.make_async_remote_copy(
            src_ref=work.at[gone], dst_ref=inbox.at[pl.ds(part * height + slots[k], sizes[k])],
            send_sem=rs_send.at[part, k], recv_sem=rs_recv.at[part, k], device_id=partner[name], device_id_type=MESH,
        )

    def ag_copy(part, k, mine):
        name = orders[part][k]
        start = bases[part][k] + (bits[name] if mine else 1 - bits[name]) * sizes[k]
        where = block(start, sizes[k])
        return pltpu.make_async_remote_copy(
            src_ref=whole.at[where], dst_ref=whole.at[where],
            send_sem=ag_send.at[part, k], recv_sem=ag_recv.at[part, k], device_id=partner[name], device_id_type=MESH,
        )

    def sm_copy(k):
        return pltpu.make_async_remote_copy(
            src_ref=small_v.at[k], dst_ref=small_in.at[k],
            send_sem=sm_send.at[k], recv_sem=sm_recv.at[k], device_id=partner[orders[0][k]], device_id_type=MESH,
        )

    small_v[0] = small_ref[...]
    for part in range(parts):
        pltpu.make_async_copy(g_ref.at[pl.ds(part * height, height)], work.at[pl.ds(part * height, height)], in_sem.at[part]).wait()
        rs_copy(part, 0).start()
    sm_copy(0).start()
    strip = 16
    for k in range(stages):
        for part in range(parts):
            rs_copy(part, k).wait_recv()
            into = whole if k == stages - 1 else work

            @pl.loop(0, sizes[k] // strip)
            def _(i, k=k, part=part, into=into):
                kept = pl.ds(pl.multiple_of(bases[part][k + 1] + i * strip, strip), strip)
                came = pl.ds(pl.multiple_of(part * height + slots[k] + i * strip, strip), strip)
                into[kept, :] = work[kept, :] + inbox[came, :]

            if k + 1 < stages:
                rs_copy(part, k + 1).start()
            else:
                ag_copy(part, k, True).start()
        sm_copy(k).wait_recv()
        if k + 1 < stages:
            small_v[k + 1] = small_v[k] + small_in[k]
            sm_copy(k + 1).start()
        else:
            small_out[...] = small_v[k] + small_in[k]

    for k in reversed(range(stages)):
        for part in range(parts):
            ag_copy(part, k, False).wait_recv()
            if k > 0:
                ag_copy(part, k - 1, True).start()
            else:
                pltpu.make_async_copy(whole.at[pl.ds(part * height, height)], out_ref.at[pl.ds(part * height, height)], out_sem.at[part]).start()

    for k in range(stages):
        for part in range(parts):
            rs_copy(part, k).wait_send()
            ag_copy(part, k, True).wait_send()
        sm_copy(k).wait_send()
    for part in range(parts):
        pltpu.make_async_copy(whole.at[pl.ds(part * height, height)], out_ref.at[pl.ds(part * height, height)], out_sem.at[part]).wait()


def total_over_devices(sums, small):
    rows, width = sums.shape
    dma = pltpu.SemaphoreType.DMA
    anywhere = pl.BlockSpec(memory_space=pl.ANY)
    vmem = pl.BlockSpec(memory_space=pltpu.VMEM)
    return pl.pallas_call(
        total_kernel,
        out_shape=(jax.ShapeDtypeStruct(sums.shape, F32), jax.ShapeDtypeStruct(small.shape, F32)),
        in_specs=[anywhere, vmem],
        out_specs=(anywhere, vmem),
        scratch_shapes=[
            pltpu.VMEM((rows, width), F32),
            pltpu.VMEM((rows, width), F32),
            pltpu.VMEM((rows, width), F32),
            pltpu.VMEM((5,) + small.shape, F32),
            pltpu.VMEM((5,) + small.shape, F32),
            dma((3, 5)), dma((3, 5)), dma((3, 5)), dma((3, 5)), dma((5,)), dma((5,)), dma((3,)), dma((3,)),
        ],
        compiler_params=pltpu.CompilerParams(collective_id=1, has_side_effects=True, vmem_limit_bytes=VMEM_LIMIT),
        name="total",
    )(sums, small)


def finish_kernel(up_ref, down_ref, proj_ref, up_out, down_out, proj_out):
    up_out[...] = up_ref[...]
    down_out[...] = down_ref[...].T
    proj_out[...] = proj_ref[...].T


def finish(sums):
    height = sums.shape[0] // 3
    wide = sums.shape[1]
    step = 512
    flat = jax.ShapeDtypeStruct((height, wide), F32)
    tall = jax.ShapeDtypeStruct((wide, height), F32)
    across = pl.BlockSpec((height, step), lambda i: (0, i))
    along = pl.BlockSpec((step, height), lambda i: (i, 0))
    return pl.pallas_call(
        finish_kernel,
        out_shape=(flat, tall, tall),
        grid=(wide // step,),
        in_specs=[pl.BlockSpec((height, step), lambda i, part=part: (part, i)) for part in range(3)],
        out_specs=(across, along, along),
        compiler_params=pltpu.CompilerParams(dimension_semantics=("arbitrary",), vmem_limit_bytes=VMEM_LIMIT),
        name="finish",
    )(sums, sums, sums)


def solution(mesh):
    dev_count = mesh.shape["data"] * mesh.shape["model"]

    def body(teacher_in, student_in, teacher_gain, teacher_up, teacher_down, student_gain, student_up, student_down, student_proj):
        seqs, tokens, t_width = teacher_in.shape
        seq_rows, seq_len, width = student_in.shape
        total = seq_rows * dev_count * seq_len * width
        grad_scale = 2.0 / total
        feature, _, _, rows = teacher_layer(
            teacher_in.reshape(seqs * tokens, t_width), teacher_gain, teacher_up[0], teacher_down[0],
            student_in.reshape(seqs, tokens, width),
        )
        sums, small = student_layer(
            jnp.full((1,), grad_scale, F32), feature, rows.reshape(seqs * tokens, width),
            student_gain, student_up[0], student_down[0], student_proj[0],
        )
        sums, small = total_over_devices(sums, small)
        grad_up, grad_down, grad_proj = finish(sums)
        loss = jnp.sum(small[1]) / total
        return (loss, grad_up[None], grad_down[None], small[None, 0], grad_proj[None])

    return jax.shard_map(
        body,
        mesh=mesh,
        in_specs=(
            P("data", "model", None),
            P(("data", "model"), None, None),
            P(),
            P(None, None, "model"),
            P(None, "model", None),
            P(),
            P(),
            P(),
            P(),
        ),
        out_specs=(P(), P(), P(), P(), P()),
        check_vma=False,
    )
```

```python
import jax
import jax.numpy as jnp
from jax import lax
from jax.experimental import pallas as pl
from jax.experimental.pallas import tpu as pltpu
from jax.sharding import PartitionSpec as P

EPS = 1e-6
MESH = pl.DeviceIdType.MESH
F32 = jnp.float32
BF16 = jnp.bfloat16
GELU_K = 0.7978845608028654
GELU_C = 0.044715
TILE = 512
CHUNK = 512
PIECES = 4
X_STEPS = (8, 18, 28, 38)
Z_DIAG_STEP = 40
STUDENT_STEP = 42
Y_DIAG_STEPS = (44, 52)
VMEM_LIMIT = 67043328


def gelu(x):
    return 0.5 * x * (1.0 + jnp.tanh(GELU_K * (x + GELU_C * (x * x * x))))


def teacher_kernel(
    h_ref, gain_ref, w1_ref, w2_ref, s_ref,
    f_ref, w1g, w2g, sx_ref,
    act, acc, w1_v, w2_v, p_a, p_b, u_a, u_b, s_v,
    x_send, x_recv, y_send, y_recv, z_send, z_recv, yd_send, yd_recv, zd_send, zd_recv,
    d_send, d_recv, g_send, g_recv, s_send, s_recv,
    w_sem, h_sem, f_sem, s_sem,
):
    data = lax.axis_index("data")
    model = lax.axis_index("model")
    y_bit = lax.rem(data, 2)
    z_bit = lax.rem(data // 2, 2)
    sib = (data, model + 1 - 2 * lax.rem(model, 2))
    x_nbr = (data, lax.rem(model + 2, 4))
    y_nbr = (data + 1 - 2 * y_bit, model)
    z_nbr = (data + 2 - 4 * z_bit, model)
    rows, width = act.shape
    quarter = w1_ref.shape[1]
    piece = CHUNK // PIECES
    n_tiles = rows // TILE
    per_quarter = quarter // CHUNK
    n_chunks = 4 * per_quarter
    chunk_x = 2 * y_bit + z_bit
    chunk_y = 2 * (1 - y_bit) + z_bit
    chunk_z = 2 * y_bit + 1 - z_bit
    chunk_d = 3 - chunk_x
    far = (chunk_x, chunk_y, chunk_z, chunk_d)

    def cols(start, size):
        return pl.ds(pl.multiple_of(start, size), size)

    def remote(src1, dst1, src2, dst2, send, recv, target):
        return (
            pltpu.make_async_remote_copy(src_ref=src1, dst_ref=dst1, send_sem=send.at[0], recv_sem=recv.at[0], device_id=target, device_id_type=MESH),
            pltpu.make_async_remote_copy(src_ref=src2, dst_ref=dst2, send_sem=send.at[1], recv_sem=recv.at[1], device_id=target, device_id_type=MESH),
        )

    def forward(chunk, p, send, recv, target):
        where = cols(chunk * CHUNK + p * piece, piece)
        return remote(w1g.at[1, :, where], w1g.at[1, :, where], w2g.at[1, where], w2g.at[1, where], send, recv, target)

    def x_copy(p):
        where = cols(chunk_x * CHUNK + p * piece, piece)
        return remote(w1_ref.at[:, where], w1g.at[1, :, where], w2_ref.at[where], w2g.at[1, where], x_send.at[p], x_recv.at[p], x_nbr)

    def y_copy(p, mine):
        return forward(chunk_x if mine else chunk_y, p, y_send.at[p], y_recv.at[p], y_nbr)

    def z_copy(p, mine):
        return forward(chunk_x if mine else chunk_z, p, z_send.at[p], z_recv.at[p], z_nbr)

    def zd_copy(p, mine):
        return forward(chunk_y if mine else chunk_d, p, zd_send.at[p], zd_recv.at[p], z_nbr)

    def yd_copy(p, mine):
        return forward(chunk_z if mine else chunk_d, p, yd_send.at[p - 2], yd_recv.at[p - 2], y_nbr)

    def d_copy(i):
        where = cols(i * CHUNK, CHUNK)
        return remote(w1_ref.at[:, where], w1g.at[0, :, where], w2_ref.at[where], w2g.at[0, where], d_send.at[i], d_recv.at[i], sib)

    def g_copy(group):
        where = cols(far[group] * CHUNK, CHUNK)
        return remote(w1g.at[1, :, where], w1g.at[2, :, where], w2g.at[1, where], w2g.at[2, where], g_send.at[group], g_recv.at[group], sib)

    def s_copy(k):
        other = lax.rem(model + k, 4)
        return pltpu.make_async_remote_copy(
            src_ref=s_ref.at[other], dst_ref=sx_ref.at[model], send_sem=s_send.at[k - 1], recv_sem=s_recv.at[k - 1],
            device_id=(data, other), device_id_type=MESH,
        )

    def s_arrival(k):
        other = lax.rem(model + 4 - k, 4)
        return pltpu.make_async_remote_copy(
            src_ref=s_ref.at[other], dst_ref=sx_ref.at[other], send_sem=s_send.at[k - 1], recv_sem=s_recv.at[k - 1],
            device_id=(data, other), device_id_type=MESH,
        )

    def load(src1, src2, slot):
        pltpu.make_async_copy(src1, w1_v.at[slot], w_sem.at[slot, 0]).start()
        pltpu.make_async_copy(src2, w2_v.at[slot], w_sem.at[slot, 1]).start()

    def load_wait(slot):
        pltpu.make_async_copy(w1_ref.at[:, pl.ds(0, CHUNK)], w1_v.at[slot], w_sem.at[slot, 0]).wait()
        pltpu.make_async_copy(w2_ref.at[pl.ds(0, CHUNK)], w2_v.at[slot], w_sem.at[slot, 1]).wait()

    def tile_rows(t):
        return pl.ds(pl.multiple_of(t * TILE, TILE), TILE)

    def h_load(t):
        return pltpu.make_async_copy(h_ref.at[tile_rows(t)], act.at[tile_rows(t)], h_sem.at[t])

    def f_store(t):
        return pltpu.make_async_copy(act.at[tile_rows(t)], f_ref.at[tile_rows(t)], f_sem.at[t])

    def take(copies):
        for copy in copies:
            copy.wait_recv()

    def give(copies):
        for copy in copies:
            copy.start()

    for t in range(n_tiles):
        h_load(t).start()
    load(w1_ref.at[:, pl.ds(0, CHUNK)], w2_ref.at[pl.ds(0, CHUNK)], 0)
    own_in = pltpu.make_async_copy(s_ref.at[model], s_v, s_sem.at[0])
    own_in.start()

    barrier = pltpu.get_barrier_semaphore()
    others = [(data, lax.rem(model + k, 4)) for k in (1, 2, 3)] + [y_nbr, z_nbr]
    for other in others:
        pl.semaphore_signal(barrier, inc=1, device_id=other, device_id_type=MESH)
    pl.semaphore_wait(barrier, len(others))

    for p in range(2):
        give(x_copy(p))
    for i in range(per_quarter):
        give(d_copy(i))

    u_a[...] = jnp.zeros_like(u_a)
    p_b[...] = jnp.zeros_like(p_b)
    sub = 64

    @pl.loop(0, n_tiles)
    def _(t):
        h_load(t).wait()

        @pl.loop(0, TILE // sub)
        def _(k):
            where = pl.ds(pl.multiple_of(t * TILE + k * sub, sub), sub)
            values = act[where, :].astype(F32)
            inv = lax.rsqrt(jnp.mean(values * values, axis=-1, keepdims=True) + EPS)
            act[where, :] = ((values * inv) * gain_ref[...]).astype(BF16)
            acc[where, :] = jnp.zeros((sub, width), F32)

    own_in.wait()
    own_out = pltpu.make_async_copy(s_v, sx_ref.at[model], s_sem.at[1])
    own_out.start()

    pairs = n_tiles // 2

    @pl.loop(0, n_chunks * pairs)
    def _(i):
        c = i // pairs
        j = lax.rem(i, pairs)
        step = 2 * i
        slot = lax.rem(c, 2)
        first = 2 * j
        before = lax.rem(first + n_tiles - 2, n_tiles)
        slot_before = jnp.where((j == 0) & (c > 0), 1 - slot, slot)

        for p in range(PIECES):

            @pl.when(step == X_STEPS[p])
            def _(p=p):
                take(x_copy(p))
                give(y_copy(p, True))
                give(z_copy(p, True))
                if p + 2 < PIECES:
                    give(x_copy(p + 2))
                if p == PIECES - 1:
                    give(g_copy(0))

        @pl.when(step == Z_DIAG_STEP)
        def _():
            for p in (0, 1):
                take(y_copy(p, False))
                give(zd_copy(p, True))

        @pl.when(step == STUDENT_STEP)
        def _():
            for k in (1, 2, 3):
                s_copy(k).start()

        for p in (2, 3):

            @pl.when(step == Y_DIAG_STEPS[p - 2])
            def _(p=p):
                take(z_copy(p, False))
                give(yd_copy(p, True))

        @pl.when(j == 0)
        def _():
            load_wait(slot)

        coming = c + 1
        loads = j == pairs - 1

        @pl.when(loads & (coming < per_quarter))
        def _():
            where = cols(coming * CHUNK, CHUNK)
            load(w1_ref.at[:, where], w2_ref.at[where], 1 - slot)

        for k in range(per_quarter):

            @pl.when(loads & (coming == per_quarter + k))
            def _(k=k):
                take(d_copy(k))
                where = cols(k * CHUNK, CHUNK)
                load(w1g.at[0, :, where], w2g.at[0, where], 1 - slot)

        for place, (group, direct) in enumerate(((0, True), (0, False), (1, True), (2, True), (1, False), (2, False), (3, True), (3, False))):

            @pl.when(loads & (coming == 2 * per_quarter + place))
            def _(group=group, direct=direct):
                if not direct:
                    take(g_copy(group))
                elif group == 1:
                    for p in (2, 3):
                        take(y_copy(p, False))
                elif group == 2:
                    for p in (0, 1):
                        take(z_copy(p, False))
                elif group == 3:
                    for p in (0, 1):
                        take(zd_copy(p, False))
                    for p in (2, 3):
                        take(yd_copy(p, False))
                if direct and group:
                    give(g_copy(group))
                where = cols(far[group] * CHUNK, CHUNK)
                source = 1 if direct else 2
                load(w1g.at[source, :, where], w2g.at[source, where], 1 - slot)

        @pl.when((c == n_chunks - 1) & (j > 0))
        def _():
            h_load(first - 2).start()
            h_load(first - 1).start()

        p_a[...] = jnp.dot(act[tile_rows(first), :], w1_v[slot], preferred_element_type=F32)
        u_b[...] = gelu(p_b[...]).astype(BF16)
        acc[tile_rows(before), :] += jnp.dot(u_a[...], w2_v[slot_before], preferred_element_type=F32)
        p_b[...] = jnp.dot(act[tile_rows(first + 1), :], w1_v[slot], preferred_element_type=F32)
        u_a[...] = gelu(p_a[...]).astype(BF16)
        acc[tile_rows(before + 1), :] += jnp.dot(u_b[...], w2_v[slot_before], preferred_element_type=F32)

    h_load(n_tiles - 2).start()
    h_load(n_tiles - 1).start()
    last = (n_chunks - 1) % 2
    u_b[...] = gelu(p_b[...]).astype(BF16)
    acc[pl.ds((n_tiles - 2) * TILE, TILE), :] += jnp.dot(u_a[...], w2_v[last], preferred_element_type=F32)
    acc[pl.ds((n_tiles - 1) * TILE, TILE), :] += jnp.dot(u_b[...], w2_v[last], preferred_element_type=F32)

    @pl.loop(0, n_tiles)
    def _(t):
        h_load(t).wait()

        @pl.loop(0, TILE // sub)
        def _(k):
            where = pl.ds(pl.multiple_of(t * TILE + k * sub, sub), sub)
            delta = acc[where, :].astype(BF16).astype(F32)
            act[where, :] = (act[where, :].astype(F32) + delta).astype(BF16)

        f_store(t).start()

    for k in (1, 2, 3):
        s_arrival(k).wait_recv()
        s_copy(k).wait_send()
    own_out.wait()
    sent = [x_copy(p) + y_copy(p, True) + z_copy(p, True) for p in range(PIECES)]
    sent += [d_copy(i) + g_copy(i) for i in range(per_quarter)]
    sent += [zd_copy(p, True) + yd_copy(p + 2, True) for p in (0, 1)]
    for copies in sent:
        for copy in copies:
            copy.wait_send()
    for t in range(n_tiles):
        f_store(t).wait()


def teacher_layer(hidden, gain, w_up, w_down, student_rows):
    rows, width = hidden.shape
    quarter = w_up.shape[1]
    per_quarter = quarter // CHUNK
    n_tiles = rows // TILE
    dma = pltpu.SemaphoreType.DMA
    anywhere = pl.BlockSpec(memory_space=pl.ANY)
    return pl.pallas_call(
        teacher_kernel,
        out_shape=(
            jax.ShapeDtypeStruct((rows, width), BF16),
            jax.ShapeDtypeStruct((3, width, quarter), BF16),
            jax.ShapeDtypeStruct((3, quarter, width), BF16),
            jax.ShapeDtypeStruct(student_rows.shape, BF16),
        ),
        in_specs=[anywhere, pl.BlockSpec(memory_space=pltpu.VMEM), anywhere, anywhere, anywhere],
        out_specs=(anywhere,) * 4,
        scratch_shapes=[
            pltpu.VMEM((rows, width), BF16),
            pltpu.VMEM((rows, width), F32),
            pltpu.VMEM((2, width, CHUNK), BF16),
            pltpu.VMEM((2, CHUNK, width), BF16),
            pltpu.VMEM((TILE, CHUNK), F32),
            pltpu.VMEM((TILE, CHUNK), F32),
            pltpu.VMEM((TILE, CHUNK), BF16),
            pltpu.VMEM((TILE, CHUNK), BF16),
            pltpu.VMEM(student_rows.shape[1:], BF16),
            *[dma((PIECES, 2))] * 6,
            *[dma((2, 2))] * 4,
            *[dma((per_quarter, 2))] * 4,
            dma((3,)), dma((3,)),
            dma((2, 2)), dma((n_tiles,)), dma((n_tiles,)), dma((2,)),
        ],
        compiler_params=pltpu.CompilerParams(collective_id=0, has_side_effects=True, vmem_limit_bytes=VMEM_LIMIT),
        cost_estimate=pl.CostEstimate(flops=16 * rows * width * quarter, bytes_accessed=8 * width * quarter * 2, transcendentals=0),
        name="teacher",
    )(hidden, gain, w_up, w_down, student_rows)


def nt_dot(a, b):
    return lax.dot_general(a, b, (((1,), (1,)), ((), ())), preferred_element_type=F32)


def tn_dot(a, b):
    return lax.dot_general(a, b, (((0,), (0,)), ((), ())), preferred_element_type=F32)


def student_kernel(scale_ref, f_ref, s_ref, gain_ref, up_ref, down_ref, proj_ref, g_ref, small_ref, pre):
    i = pl.program_id(0)
    width = s_ref.shape[1]
    scale = scale_ref[0]

    @pl.when(i == 0)
    def _():
        g_ref[...] = jnp.zeros_like(g_ref)
        small_ref[...] = jnp.zeros_like(small_ref)

    state = s_ref[...].astype(F32)
    normed = state * lax.rsqrt(jnp.mean(state * state, axis=-1, keepdims=True) + EPS)
    act_in = (normed * gain_ref[...]).astype(BF16)
    pre[...] = jnp.dot(act_in, up_ref[...], preferred_element_type=F32)
    up_act = gelu(pre[...]).astype(BF16)
    new_state = (state + jnp.dot(up_act, down_ref[...], preferred_element_type=F32)).astype(BF16).astype(F32)
    target = jnp.dot(f_ref[...], proj_ref[...], preferred_element_type=F32).astype(BF16).astype(F32)
    inv = lax.rsqrt(jnp.mean(new_state * new_state, axis=-1, keepdims=True) + EPS)
    unit = new_state * inv
    error = target - unit
    grad = -scale * error
    d_res = inv * (grad - unit * jnp.mean(grad * unit, axis=-1, keepdims=True))
    d_out = d_res.astype(BF16)
    g_ref[pl.ds(2 * width, width), :] += scale * tn_dot(error.astype(BF16), f_ref[...])
    g_ref[pl.ds(width, width), :] += tn_dot(d_out, up_act)
    d_up = nt_dot(d_out, down_ref[...])
    x = pre[...]
    x2 = x * x
    th = jnp.tanh(GELU_K * (x + GELU_C * (x2 * x)))
    slope = 0.5 * (1.0 + th) + 0.5 * x * (1.0 - th * th) * (GELU_K * (1.0 + 3.0 * GELU_C * x2))
    d_pre = (slope * d_up).astype(BF16)
    g_ref[pl.ds(0, width), :] += tn_dot(act_in, d_pre)
    d_act = nt_dot(d_pre, up_ref[...])
    small_ref[pl.ds(0, 1), :] += jnp.sum(d_act * normed, axis=0, keepdims=True)
    squares = jnp.sum(error * error, axis=0, keepdims=True)
    small_ref[pl.ds(1, 1), :] += squares


def student_layer(scale, feature, student_rows, gain, w_up, w_down, proj):
    rows, t_width = feature.shape
    width = student_rows.shape[1]
    wide = w_up.shape[1]
    tile = 512
    whole = pl.BlockSpec(memory_space=pltpu.VMEM)
    return pl.pallas_call(
        student_kernel,
        out_shape=(jax.ShapeDtypeStruct((3 * width, wide), F32), jax.ShapeDtypeStruct((8, width), F32)),
        grid=(rows // tile,),
        in_specs=[
            pl.BlockSpec(memory_space=pltpu.SMEM),
            pl.BlockSpec((tile, t_width), lambda i: (i, 0)),
            pl.BlockSpec((tile, width), lambda i: (i, 0)),
            whole, whole, whole, whole,
        ],
        out_specs=(pl.BlockSpec(memory_space=pltpu.VMEM),) * 2,
        scratch_shapes=[pltpu.VMEM((tile, wide), F32)],
        compiler_params=pltpu.CompilerParams(dimension_semantics=("arbitrary",), vmem_limit_bytes=VMEM_LIMIT),
        cost_estimate=pl.CostEstimate(flops=12 * rows * width * wide + 4 * rows * width * t_width, bytes_accessed=2 * rows * (t_width + width), transcendentals=0),
        name="student",
    )(scale, feature, student_rows, gain, w_up, w_down, proj)


def total_kernel(
    g_ref, small_ref, out_ref, small_out,
    work, inbox, whole, packed, came_in, small_v, small_in,
    rs_send, rs_recv, ag_send, ag_recv, sm_send, sm_recv, in_sem, out_sem,
):
    data = lax.axis_index("data")
    model = lax.axis_index("model")
    bits = {
        "core": lax.rem(model, 2),
        "x": model // 2,
        "y": lax.rem(data, 2),
        "z": lax.rem(data // 2, 2),
        "zz": data // 4,
    }
    turn = {name: 1 - 2 * bit for name, bit in bits.items()}
    partner = {
        "core": (data, model + turn["core"]),
        "x": (data, model + 2 * turn["x"]),
        "y": (data + turn["y"], model),
        "z": (data + 2 * turn["z"], model),
        "zz": (data + 4 * turn["zz"], model),
    }
    orders = (("core", "x", "y", "z", "zz"), ("core", "y", "z", "x", "zz"), ("core", "z", "x", "y", "zz"))
    stages = len(orders[0])
    parts = len(orders)
    height = work.shape[0] // parts
    sizes = [height >> (k + 1) for k in range(stages)]
    slots = [height - (height >> k) for k in range(stages)]

    def block(start, size):
        return pl.ds(pl.multiple_of(start, size), size)

    for part in range(parts):
        pltpu.make_async_copy(g_ref.at[pl.ds(part * height, height)], work.at[pl.ds(part * height, height)], in_sem.at[part]).start()

    barrier = pltpu.get_barrier_semaphore()
    for target in partner.values():
        pl.semaphore_signal(barrier, inc=1, device_id=target, device_id_type=MESH)
    pl.semaphore_wait(barrier, stages)

    bases = [[part * height] for part in range(parts)]
    for part in range(parts):
        for k in range(stages):
            bases[part].append(bases[part][k] + bits[orders[part][k]] * sizes[k])

    def rs_copy(part, k):
        name = orders[part][k]
        gone = block(bases[part][k] + (1 - bits[name]) * sizes[k], sizes[k])
        if k == 0:
            source, target = work.at[gone], inbox.at[pl.ds(part * sizes[0], sizes[0])]
        else:
            where = pl.ds(part * sizes[0] + slots[k] - slots[1], sizes[k])
            source, target = packed.at[where], came_in.at[where]
        return pltpu.make_async_remote_copy(
            src_ref=source, dst_ref=target,
            send_sem=rs_send.at[part, k], recv_sem=rs_recv.at[part, k], device_id=partner[name], device_id_type=MESH,
        )

    def ag_copy(part, k, mine):
        name = orders[part][k]
        start = bases[part][k] + (bits[name] if mine else 1 - bits[name]) * sizes[k]
        where = block(start, sizes[k])
        return pltpu.make_async_remote_copy(
            src_ref=whole.at[where], dst_ref=whole.at[where],
            send_sem=ag_send.at[part, k], recv_sem=ag_recv.at[part, k], device_id=partner[name], device_id_type=MESH,
        )

    def sm_copy(k):
        return pltpu.make_async_remote_copy(
            src_ref=small_v.at[k], dst_ref=small_in.at[k],
            send_sem=sm_send.at[k], recv_sem=sm_recv.at[k], device_id=partner[orders[0][k]], device_id_type=MESH,
        )

    small_v[0] = small_ref[...]
    for part in range(parts):
        pltpu.make_async_copy(g_ref.at[pl.ds(part * height, height)], work.at[pl.ds(part * height, height)], in_sem.at[part]).wait()
        rs_copy(part, 0).start()
    sm_copy(0).start()
    strip = 16
    for k in range(stages):
        for part in range(parts):
            rs_copy(part, k).wait_recv()
            into = whole if k == stages - 1 else work

            @pl.loop(0, sizes[k] // strip)
            def _(i, k=k, part=part, into=into):
                kept = pl.ds(pl.multiple_of(bases[part][k + 1] + i * strip, strip), strip)
                box, low = (inbox, 0) if k == 0 else (came_in, slots[k] - slots[1])
                came = pl.ds(pl.multiple_of(part * sizes[0] + low + i * strip, strip), strip)
                into[kept, :] = work[kept, :] + box[came, :].astype(F32)

            if k + 1 < stages:
                name = orders[part][k + 1]
                gone = bases[part][k + 1] + (1 - bits[name]) * sizes[k + 1]
                low = part * sizes[0] + slots[k + 1] - slots[1]

                @pl.loop(0, sizes[k + 1] // strip)
                def _(i, gone=gone, low=low):
                    source = pl.ds(pl.multiple_of(gone + i * strip, strip), strip)
                    packed[pl.ds(pl.multiple_of(low + i * strip, strip), strip), :] = work[source, :].astype(BF16)

                rs_copy(part, k + 1).start()
            else:
                ag_copy(part, k, True).start()
        sm_copy(k).wait_recv()
        if k + 1 < stages:
            small_v[k + 1] = small_v[k] + small_in[k]
            sm_copy(k + 1).start()
        else:
            small_out[...] = small_v[k] + small_in[k]

    for k in reversed(range(stages)):
        for part in range(parts):
            ag_copy(part, k, False).wait_recv()
            if k > 0:
                ag_copy(part, k - 1, True).start()
            else:
                pltpu.make_async_copy(whole.at[pl.ds(part * height, height)], out_ref.at[pl.ds(part * height, height)], out_sem.at[part]).start()

    for k in range(stages):
        for part in range(parts):
            rs_copy(part, k).wait_send()
            ag_copy(part, k, True).wait_send()
        sm_copy(k).wait_send()
    for part in range(parts):
        pltpu.make_async_copy(whole.at[pl.ds(part * height, height)], out_ref.at[pl.ds(part * height, height)], out_sem.at[part]).wait()


def total_over_devices(sums, small):
    rows, width = sums.shape
    dma = pltpu.SemaphoreType.DMA
    anywhere = pl.BlockSpec(memory_space=pl.ANY)
    vmem = pl.BlockSpec(memory_space=pltpu.VMEM)
    return pl.pallas_call(
        total_kernel,
        out_shape=(jax.ShapeDtypeStruct(sums.shape, F32), jax.ShapeDtypeStruct(small.shape, F32)),
        in_specs=[anywhere, vmem],
        out_specs=(anywhere, vmem),
        scratch_shapes=[
            pltpu.VMEM((rows, width), F32),
            pltpu.VMEM((rows // 2, width), F32),
            pltpu.VMEM((rows, width), F32),
            pltpu.VMEM((rows // 2, width), BF16),
            pltpu.VMEM((rows // 2, width), BF16),
            pltpu.VMEM((5,) + small.shape, F32),
            pltpu.VMEM((5,) + small.shape, F32),
            dma((3, 5)), dma((3, 5)), dma((3, 5)), dma((3, 5)), dma((5,)), dma((5,)), dma((3,)), dma((3,)),
        ],
        compiler_params=pltpu.CompilerParams(collective_id=1, has_side_effects=True, vmem_limit_bytes=VMEM_LIMIT),
        name="total",
    )(sums, small)


def finish_kernel(up_ref, down_ref, proj_ref, up_out, down_out, proj_out):
    up_out[...] = up_ref[...]
    down_out[...] = down_ref[...].T
    proj_out[...] = proj_ref[...].T


def finish(sums):
    height = sums.shape[0] // 3
    wide = sums.shape[1]
    step = 512
    flat = jax.ShapeDtypeStruct((height, wide), F32)
    tall = jax.ShapeDtypeStruct((wide, height), F32)
    across = pl.BlockSpec((height, step), lambda i: (0, i))
    along = pl.BlockSpec((step, height), lambda i: (i, 0))
    return pl.pallas_call(
        finish_kernel,
        out_shape=(flat, tall, tall),
        grid=(wide // step,),
        in_specs=[pl.BlockSpec((height, step), lambda i, part=part: (part, i)) for part in range(3)],
        out_specs=(across, along, along),
        compiler_params=pltpu.CompilerParams(dimension_semantics=("arbitrary",), vmem_limit_bytes=VMEM_LIMIT),
        name="finish",
    )(sums, sums, sums)


def solution(mesh):
    dev_count = mesh.shape["data"] * mesh.shape["model"]

    def body(teacher_in, student_in, teacher_gain, teacher_up, teacher_down, student_gain, student_up, student_down, student_proj):
        seqs, tokens, t_width = teacher_in.shape
        seq_rows, seq_len, width = student_in.shape
        total = seq_rows * dev_count * seq_len * width
        grad_scale = 2.0 / total
        feature, _, _, rows = teacher_layer(
            teacher_in.reshape(seqs * tokens, t_width), teacher_gain, teacher_up[0], teacher_down[0],
            student_in.reshape(seqs, tokens, width),
        )
        sums, small = student_layer(
            jnp.full((1,), grad_scale, F32), feature, rows.reshape(seqs * tokens, width),
            student_gain, student_up[0], student_down[0], student_proj[0],
        )
        sums, small = total_over_devices(sums, small)
        grad_up, grad_down, grad_proj = finish(sums)
        loss = jnp.sum(small[1]) / total
        return (loss, grad_up[None], grad_down[None], small[None, 0], grad_proj[None])

    return jax.shard_map(
        body,
        mesh=mesh,
        in_specs=(
            P("data", "model", None),
            P(("data", "model"), None, None),
            P(),
            P(None, None, "model"),
            P(None, "model", None),
            P(),
            P(),
            P(),
            P(),
        ),
        out_specs=(P(), P(), P(), P(), P()),
        check_vma=False,
    )
```

```python
import jax
import jax.numpy as jnp
from jax import lax
from jax.experimental import pallas as pl
from jax.experimental.pallas import tpu as pltpu
from jax.sharding import PartitionSpec as P

EPS = 1e-6
MESH = pl.DeviceIdType.MESH
F32 = jnp.float32
BF16 = jnp.bfloat16
GELU_K = 0.7978845608028654
GELU_C = 0.044715
TILE = 512
CHUNK = 512
PIECES = 4
X_STEPS = (8, 18, 28, 38)
Z_DIAG_STEP = 40
STUDENT_STEP = 42
Y_DIAG_STEPS = (44, 52)
VMEM_LIMIT = 67043328


def gelu(x):
    half = 0.5 * x
    return half + half * jnp.tanh(x * (GELU_K + (GELU_K * GELU_C) * (x * x)))


def teacher_kernel(
    h_ref, gain_ref, w1_ref, w2_ref, s_ref,
    f_ref, w1g, w2g, sx_ref,
    act, acc, w1_v, w2_v, p_a, p_b, u_a, u_b, s_v,
    x_send, x_recv, y_send, y_recv, z_send, z_recv, yd_send, yd_recv, zd_send, zd_recv,
    d_send, d_recv, g_send, g_recv, s_send, s_recv,
    w_sem, h_sem, f_sem, s_sem,
):
    data = lax.axis_index("data")
    model = lax.axis_index("model")
    y_bit = lax.rem(data, 2)
    z_bit = lax.rem(data // 2, 2)
    sib = (data, model + 1 - 2 * lax.rem(model, 2))
    x_nbr = (data, lax.rem(model + 2, 4))
    y_nbr = (data + 1 - 2 * y_bit, model)
    z_nbr = (data + 2 - 4 * z_bit, model)
    rows, width = act.shape
    quarter = w1_ref.shape[1]
    piece = CHUNK // PIECES
    n_tiles = rows // TILE
    per_quarter = quarter // CHUNK
    n_chunks = 4 * per_quarter
    chunk_x = 2 * y_bit + z_bit
    chunk_y = 2 * (1 - y_bit) + z_bit
    chunk_z = 2 * y_bit + 1 - z_bit
    chunk_d = 3 - chunk_x
    far = (chunk_x, chunk_y, chunk_z, chunk_d)

    def cols(start, size):
        return pl.ds(pl.multiple_of(start, size), size)

    def remote(src1, dst1, src2, dst2, send, recv, target):
        return (
            pltpu.make_async_remote_copy(src_ref=src1, dst_ref=dst1, send_sem=send.at[0], recv_sem=recv.at[0], device_id=target, device_id_type=MESH),
            pltpu.make_async_remote_copy(src_ref=src2, dst_ref=dst2, send_sem=send.at[1], recv_sem=recv.at[1], device_id=target, device_id_type=MESH),
        )

    def forward(chunk, p, send, recv, target):
        where = cols(chunk * CHUNK + p * piece, piece)
        return remote(w1g.at[1, :, where], w1g.at[1, :, where], w2g.at[1, where], w2g.at[1, where], send, recv, target)

    def x_copy(p):
        where = cols(chunk_x * CHUNK + p * piece, piece)
        return remote(w1_ref.at[:, where], w1g.at[1, :, where], w2_ref.at[where], w2g.at[1, where], x_send.at[p], x_recv.at[p], x_nbr)

    def y_copy(p, mine):
        return forward(chunk_x if mine else chunk_y, p, y_send.at[p], y_recv.at[p], y_nbr)

    def z_copy(p, mine):
        return forward(chunk_x if mine else chunk_z, p, z_send.at[p], z_recv.at[p], z_nbr)

    def zd_copy(p, mine):
        return forward(chunk_y if mine else chunk_d, p, zd_send.at[p], zd_recv.at[p], z_nbr)

    def yd_copy(p, mine):
        return forward(chunk_z if mine else chunk_d, p, yd_send.at[p - 2], yd_recv.at[p - 2], y_nbr)

    def d_copy(i):
        where = cols(i * CHUNK, CHUNK)
        return remote(w1_ref.at[:, where], w1g.at[0, :, where], w2_ref.at[where], w2g.at[0, where], d_send.at[i], d_recv.at[i], sib)

    def g_copy(group):
        where = cols(far[group] * CHUNK, CHUNK)
        return remote(w1g.at[1, :, where], w1g.at[2, :, where], w2g.at[1, where], w2g.at[2, where], g_send.at[group], g_recv.at[group], sib)

    def s_copy(k):
        other = lax.rem(model + k, 4)
        return pltpu.make_async_remote_copy(
            src_ref=s_ref.at[other], dst_ref=sx_ref.at[model], send_sem=s_send.at[k - 1], recv_sem=s_recv.at[k - 1],
            device_id=(data, other), device_id_type=MESH,
        )

    def s_arrival(k):
        other = lax.rem(model + 4 - k, 4)
        return pltpu.make_async_remote_copy(
            src_ref=s_ref.at[other], dst_ref=sx_ref.at[other], send_sem=s_send.at[k - 1], recv_sem=s_recv.at[k - 1],
            device_id=(data, other), device_id_type=MESH,
        )

    def load(src1, src2, slot):
        pltpu.make_async_copy(src1, w1_v.at[slot], w_sem.at[slot, 0]).start()
        pltpu.make_async_copy(src2, w2_v.at[slot], w_sem.at[slot, 1]).start()

    def load_wait(slot):
        pltpu.make_async_copy(w1_ref.at[:, pl.ds(0, CHUNK)], w1_v.at[slot], w_sem.at[slot, 0]).wait()
        pltpu.make_async_copy(w2_ref.at[pl.ds(0, CHUNK)], w2_v.at[slot], w_sem.at[slot, 1]).wait()

    def tile_rows(t):
        return pl.ds(pl.multiple_of(t * TILE, TILE), TILE)

    def h_load(t):
        return pltpu.make_async_copy(h_ref.at[tile_rows(t)], act.at[tile_rows(t)], h_sem.at[t])

    def f_store(t):
        return pltpu.make_async_copy(act.at[tile_rows(t)], f_ref.at[tile_rows(t)], f_sem.at[t])

    def take(copies):
        for copy in copies:
            copy.wait_recv()

    def give(copies):
        for copy in copies:
            copy.start()

    for t in range(n_tiles):
        h_load(t).start()
    load(w1_ref.at[:, pl.ds(0, CHUNK)], w2_ref.at[pl.ds(0, CHUNK)], 0)
    own_in = pltpu.make_async_copy(s_ref.at[model], s_v, s_sem.at[0])
    own_in.start()

    barrier = pltpu.get_barrier_semaphore()
    others = [(data, lax.rem(model + k, 4)) for k in (1, 2, 3)] + [y_nbr, z_nbr]
    for other in others:
        pl.semaphore_signal(barrier, inc=1, device_id=other, device_id_type=MESH)
    pl.semaphore_wait(barrier, len(others))

    for p in range(2):
        give(x_copy(p))
    for i in range(per_quarter):
        give(d_copy(i))

    u_a[...] = jnp.zeros_like(u_a)
    p_b[...] = jnp.zeros_like(p_b)
    sub = 64

    @pl.loop(0, n_tiles)
    def _(t):
        h_load(t).wait()

        @pl.loop(0, TILE // sub)
        def _(k):
            where = pl.ds(pl.multiple_of(t * TILE + k * sub, sub), sub)
            values = act[where, :].astype(F32)
            inv = lax.rsqrt(jnp.mean(values * values, axis=-1, keepdims=True) + EPS)
            act[where, :] = ((values * inv) * gain_ref[...]).astype(BF16)
            acc[where, :] = jnp.zeros((sub, width), F32)

    own_in.wait()
    own_out = pltpu.make_async_copy(s_v, sx_ref.at[model], s_sem.at[1])
    own_out.start()

    pairs = n_tiles // 2

    @pl.loop(0, n_chunks * pairs)
    def _(i):
        c = i // pairs
        j = lax.rem(i, pairs)
        step = 2 * i
        slot = lax.rem(c, 2)
        first = 2 * j
        before = lax.rem(first + n_tiles - 2, n_tiles)
        slot_before = jnp.where((j == 0) & (c > 0), 1 - slot, slot)

        for p in range(PIECES):

            @pl.when(step == X_STEPS[p])
            def _(p=p):
                take(x_copy(p))
                give(y_copy(p, True))
                give(z_copy(p, True))
                if p + 2 < PIECES:
                    give(x_copy(p + 2))
                if p == PIECES - 1:
                    give(g_copy(0))

        @pl.when(step == Z_DIAG_STEP)
        def _():
            for p in (0, 1):
                take(y_copy(p, False))
                give(zd_copy(p, True))

        @pl.when(step == STUDENT_STEP)
        def _():
            for k in (1, 2, 3):
                s_copy(k).start()

        for p in (2, 3):

            @pl.when(step == Y_DIAG_STEPS[p - 2])
            def _(p=p):
                take(z_copy(p, False))
                give(yd_copy(p, True))

        @pl.when(j == 0)
        def _():
            load_wait(slot)

        coming = c + 1
        loads = j == pairs - 1

        @pl.when(loads & (coming < per_quarter))
        def _():
            where = cols(coming * CHUNK, CHUNK)
            load(w1_ref.at[:, where], w2_ref.at[where], 1 - slot)

        for k in range(per_quarter):

            @pl.when(loads & (coming == per_quarter + k))
            def _(k=k):
                take(d_copy(k))
                where = cols(k * CHUNK, CHUNK)
                load(w1g.at[0, :, where], w2g.at[0, where], 1 - slot)

        for place, (group, direct) in enumerate(((0, True), (0, False), (1, True), (2, True), (1, False), (2, False), (3, True), (3, False))):

            @pl.when(loads & (coming == 2 * per_quarter + place))
            def _(group=group, direct=direct):
                if not direct:
                    take(g_copy(group))
                elif group == 1:
                    for p in (2, 3):
                        take(y_copy(p, False))
                elif group == 2:
                    for p in (0, 1):
                        take(z_copy(p, False))
                elif group == 3:
                    for p in (0, 1):
                        take(zd_copy(p, False))
                    for p in (2, 3):
                        take(yd_copy(p, False))
                if direct and group:
                    give(g_copy(group))
                where = cols(far[group] * CHUNK, CHUNK)
                source = 1 if direct else 2
                load(w1g.at[source, :, where], w2g.at[source, where], 1 - slot)

        @pl.when((c == n_chunks - 1) & (j > 0))
        def _():
            h_load(first - 2).start()
            h_load(first - 1).start()

        p_a[...] = jnp.dot(act[tile_rows(first), :], w1_v[slot], preferred_element_type=F32)
        u_b[...] = gelu(p_b[...]).astype(BF16)
        acc[tile_rows(before), :] += jnp.dot(u_a[...], w2_v[slot_before], preferred_element_type=F32)
        p_b[...] = jnp.dot(act[tile_rows(first + 1), :], w1_v[slot], preferred_element_type=F32)
        u_a[...] = gelu(p_a[...]).astype(BF16)
        acc[tile_rows(before + 1), :] += jnp.dot(u_b[...], w2_v[slot_before], preferred_element_type=F32)

    h_load(n_tiles - 2).start()
    h_load(n_tiles - 1).start()
    last = (n_chunks - 1) % 2
    u_b[...] = gelu(p_b[...]).astype(BF16)
    acc[pl.ds((n_tiles - 2) * TILE, TILE), :] += jnp.dot(u_a[...], w2_v[last], preferred_element_type=F32)
    acc[pl.ds((n_tiles - 1) * TILE, TILE), :] += jnp.dot(u_b[...], w2_v[last], preferred_element_type=F32)

    @pl.loop(0, n_tiles)
    def _(t):
        h_load(t).wait()

        @pl.loop(0, TILE // sub)
        def _(k):
            where = pl.ds(pl.multiple_of(t * TILE + k * sub, sub), sub)
            delta = acc[where, :].astype(BF16).astype(F32)
            act[where, :] = (act[where, :].astype(F32) + delta).astype(BF16)

        f_store(t).start()

    for k in (1, 2, 3):
        s_arrival(k).wait_recv()
        s_copy(k).wait_send()
    own_out.wait()
    sent = [x_copy(p) + y_copy(p, True) + z_copy(p, True) for p in range(PIECES)]
    sent += [d_copy(i) + g_copy(i) for i in range(per_quarter)]
    sent += [zd_copy(p, True) + yd_copy(p + 2, True) for p in (0, 1)]
    for copies in sent:
        for copy in copies:
            copy.wait_send()
    for t in range(n_tiles):
        f_store(t).wait()


def teacher_layer(hidden, gain, w_up, w_down, student_rows):
    rows, width = hidden.shape
    quarter = w_up.shape[1]
    per_quarter = quarter // CHUNK
    n_tiles = rows // TILE
    dma = pltpu.SemaphoreType.DMA
    anywhere = pl.BlockSpec(memory_space=pl.ANY)
    return pl.pallas_call(
        teacher_kernel,
        out_shape=(
            jax.ShapeDtypeStruct((rows, width), BF16),
            jax.ShapeDtypeStruct((3, width, quarter), BF16),
            jax.ShapeDtypeStruct((3, quarter, width), BF16),
            jax.ShapeDtypeStruct(student_rows.shape, BF16),
        ),
        in_specs=[anywhere, pl.BlockSpec(memory_space=pltpu.VMEM), anywhere, anywhere, anywhere],
        out_specs=(anywhere,) * 4,
        scratch_shapes=[
            pltpu.VMEM((rows, width), BF16),
            pltpu.VMEM((rows, width), F32),
            pltpu.VMEM((2, width, CHUNK), BF16),
            pltpu.VMEM((2, CHUNK, width), BF16),
            pltpu.VMEM((TILE, CHUNK), F32),
            pltpu.VMEM((TILE, CHUNK), F32),
            pltpu.VMEM((TILE, CHUNK), BF16),
            pltpu.VMEM((TILE, CHUNK), BF16),
            pltpu.VMEM(student_rows.shape[1:], BF16),
            *[dma((PIECES, 2))] * 6,
            *[dma((2, 2))] * 4,
            *[dma((per_quarter, 2))] * 4,
            dma((3,)), dma((3,)),
            dma((2, 2)), dma((n_tiles,)), dma((n_tiles,)), dma((2,)),
        ],
        compiler_params=pltpu.CompilerParams(collective_id=0, has_side_effects=True, vmem_limit_bytes=VMEM_LIMIT),
        cost_estimate=pl.CostEstimate(flops=16 * rows * width * quarter, bytes_accessed=8 * width * quarter * 2, transcendentals=0),
        name="teacher",
    )(hidden, gain, w_up, w_down, student_rows)


def nt_dot(a, b):
    return lax.dot_general(a, b, (((1,), (1,)), ((), ())), preferred_element_type=F32)


def tn_dot(a, b):
    return lax.dot_general(a, b, (((0,), (0,)), ((), ())), preferred_element_type=F32)


def student_kernel(scale_ref, f_ref, s_ref, gain_ref, up_ref, down_ref, proj_ref, g_ref, small_ref, slope):
    i = pl.program_id(0)
    width = s_ref.shape[1]
    scale = scale_ref[0]

    @pl.when(i == 0)
    def _():
        g_ref[...] = jnp.zeros_like(g_ref)
        small_ref[...] = jnp.zeros_like(small_ref)

    state = s_ref[...].astype(F32)
    normed = state * lax.rsqrt(jnp.mean(state * state, axis=-1, keepdims=True) + EPS)
    act_in = (normed * gain_ref[...]).astype(BF16)
    pre = jnp.dot(act_in, up_ref[...], preferred_element_type=F32)
    half = 0.5 * pre
    cubic = (GELU_K * GELU_C) * (pre * pre)
    th = jnp.tanh(pre * (GELU_K + cubic))
    up_act = (half + half * th).astype(BF16)
    slope[...] = (0.5 + 0.5 * th) + (half * (1.0 - th * th)) * (GELU_K + 3.0 * cubic)
    new_state = (state + jnp.dot(up_act, down_ref[...], preferred_element_type=F32)).astype(BF16).astype(F32)
    target = jnp.dot(f_ref[...], proj_ref[...], preferred_element_type=F32).astype(BF16).astype(F32)
    inv = lax.rsqrt(jnp.mean(new_state * new_state, axis=-1, keepdims=True) + EPS)
    unit = new_state * inv
    error = target - unit
    grad = -scale * error
    d_res = inv * (grad - unit * jnp.mean(grad * unit, axis=-1, keepdims=True))
    d_out = d_res.astype(BF16)
    g_ref[pl.ds(2 * width, width), :] += scale * tn_dot(error.astype(BF16), f_ref[...])
    g_ref[pl.ds(width, width), :] += tn_dot(d_out, up_act)
    d_up = nt_dot(d_out, down_ref[...])
    d_pre = (slope[...] * d_up).astype(BF16)
    g_ref[pl.ds(0, width), :] += tn_dot(act_in, d_pre)
    d_act = nt_dot(d_pre, up_ref[...])
    small_ref[pl.ds(0, 1), :] += jnp.sum(d_act * normed, axis=0, keepdims=True)
    squares = jnp.sum(error * error, axis=0, keepdims=True)
    small_ref[pl.ds(1, 1), :] += squares


def student_layer(scale, feature, student_rows, gain, w_up, w_down, proj):
    rows, t_width = feature.shape
    width = student_rows.shape[1]
    wide = w_up.shape[1]
    tile = 512
    whole = pl.BlockSpec(memory_space=pltpu.VMEM)
    return pl.pallas_call(
        student_kernel,
        out_shape=(jax.ShapeDtypeStruct((3 * width, wide), F32), jax.ShapeDtypeStruct((8, width), F32)),
        grid=(rows // tile,),
        in_specs=[
            pl.BlockSpec(memory_space=pltpu.SMEM),
            pl.BlockSpec((tile, t_width), lambda i: (i, 0)),
            pl.BlockSpec((tile, width), lambda i: (i, 0)),
            whole, whole, whole, whole,
        ],
        out_specs=(pl.BlockSpec(memory_space=pltpu.VMEM),) * 2,
        scratch_shapes=[pltpu.VMEM((tile, wide), F32)],
        compiler_params=pltpu.CompilerParams(dimension_semantics=("arbitrary",), vmem_limit_bytes=VMEM_LIMIT),
        cost_estimate=pl.CostEstimate(flops=12 * rows * width * wide + 4 * rows * width * t_width, bytes_accessed=2 * rows * (t_width + width), transcendentals=0),
        name="student",
    )(scale, feature, student_rows, gain, w_up, w_down, proj)


def total_kernel(
    g_ref, small_ref, out_ref, small_out,
    work, inbox, whole, packed, came_in, small_v, small_in,
    rs_send, rs_recv, ag_send, ag_recv, sm_send, sm_recv, in_sem, out_sem,
):
    data = lax.axis_index("data")
    model = lax.axis_index("model")
    bits = {
        "core": lax.rem(model, 2),
        "x": model // 2,
        "y": lax.rem(data, 2),
        "z": lax.rem(data // 2, 2),
        "zz": data // 4,
    }
    turn = {name: 1 - 2 * bit for name, bit in bits.items()}
    partner = {
        "core": (data, model + turn["core"]),
        "x": (data, model + 2 * turn["x"]),
        "y": (data + turn["y"], model),
        "z": (data + 2 * turn["z"], model),
        "zz": (data + 4 * turn["zz"], model),
    }
    orders = (("core", "x", "y", "z", "zz"), ("core", "y", "z", "x", "zz"), ("core", "z", "x", "y", "zz"))
    stages = len(orders[0])
    parts = len(orders)
    height = work.shape[0] // parts
    sizes = [height >> (k + 1) for k in range(stages)]
    slots = [height - (height >> k) for k in range(stages)]

    def block(start, size):
        return pl.ds(pl.multiple_of(start, size), size)

    for part in range(parts):
        pltpu.make_async_copy(g_ref.at[pl.ds(part * height, height)], work.at[pl.ds(part * height, height)], in_sem.at[part]).start()

    barrier = pltpu.get_barrier_semaphore()
    for target in partner.values():
        pl.semaphore_signal(barrier, inc=1, device_id=target, device_id_type=MESH)
    pl.semaphore_wait(barrier, stages)

    bases = [[part * height] for part in range(parts)]
    for part in range(parts):
        for k in range(stages):
            bases[part].append(bases[part][k] + bits[orders[part][k]] * sizes[k])

    def rs_copy(part, k):
        name = orders[part][k]
        gone = block(bases[part][k] + (1 - bits[name]) * sizes[k], sizes[k])
        if k == 0:
            source, target = work.at[gone], inbox.at[pl.ds(part * sizes[0], sizes[0])]
        else:
            where = pl.ds(part * sizes[0] + slots[k] - slots[1], sizes[k])
            source, target = packed.at[where], came_in.at[where]
        return pltpu.make_async_remote_copy(
            src_ref=source, dst_ref=target,
            send_sem=rs_send.at[part, k], recv_sem=rs_recv.at[part, k], device_id=partner[name], device_id_type=MESH,
        )

    def ag_copy(part, k, mine):
        name = orders[part][k]
        start = bases[part][k] + (bits[name] if mine else 1 - bits[name]) * sizes[k]
        where = block(start, sizes[k])
        return pltpu.make_async_remote_copy(
            src_ref=whole.at[where], dst_ref=whole.at[where],
            send_sem=ag_send.at[part, k], recv_sem=ag_recv.at[part, k], device_id=partner[name], device_id_type=MESH,
        )

    def sm_copy(k):
        return pltpu.make_async_remote_copy(
            src_ref=small_v.at[k], dst_ref=small_in.at[k],
            send_sem=sm_send.at[k], recv_sem=sm_recv.at[k], device_id=partner[orders[0][k]], device_id_type=MESH,
        )

    small_v[0] = small_ref[...]
    for part in range(parts):
        pltpu.make_async_copy(g_ref.at[pl.ds(part * height, height)], work.at[pl.ds(part * height, height)], in_sem.at[part]).wait()
        rs_copy(part, 0).start()
    sm_copy(0).start()
    strip = 16
    for k in range(stages):
        for part in range(parts):
            rs_copy(part, k).wait_recv()
            into = whole if k == stages - 1 else work

            @pl.loop(0, sizes[k] // strip)
            def _(i, k=k, part=part, into=into):
                kept = pl.ds(pl.multiple_of(bases[part][k + 1] + i * strip, strip), strip)
                box, low = (inbox, 0) if k == 0 else (came_in, slots[k] - slots[1])
                came = pl.ds(pl.multiple_of(part * sizes[0] + low + i * strip, strip), strip)
                into[kept, :] = work[kept, :] + box[came, :].astype(F32)

            if k + 1 < stages:
                name = orders[part][k + 1]
                gone = bases[part][k + 1] + (1 - bits[name]) * sizes[k + 1]
                low = part * sizes[0] + slots[k + 1] - slots[1]

                @pl.loop(0, sizes[k + 1] // strip)
                def _(i, gone=gone, low=low):
                    source = pl.ds(pl.multiple_of(gone + i * strip, strip), strip)
                    packed[pl.ds(pl.multiple_of(low + i * strip, strip), strip), :] = work[source, :].astype(BF16)

                rs_copy(part, k + 1).start()
            else:
                ag_copy(part, k, True).start()
        sm_copy(k).wait_recv()
        if k + 1 < stages:
            small_v[k + 1] = small_v[k] + small_in[k]
            sm_copy(k + 1).start()
        else:
            small_out[...] = small_v[k] + small_in[k]

    for k in reversed(range(stages)):
        for part in range(parts):
            ag_copy(part, k, False).wait_recv()
            if k > 0:
                ag_copy(part, k - 1, True).start()
            else:
                pltpu.make_async_copy(whole.at[pl.ds(part * height, height)], out_ref.at[pl.ds(part * height, height)], out_sem.at[part]).start()

    for k in range(stages):
        for part in range(parts):
            rs_copy(part, k).wait_send()
            ag_copy(part, k, True).wait_send()
        sm_copy(k).wait_send()
    for part in range(parts):
        pltpu.make_async_copy(whole.at[pl.ds(part * height, height)], out_ref.at[pl.ds(part * height, height)], out_sem.at[part]).wait()


def total_over_devices(sums, small):
    rows, width = sums.shape
    dma = pltpu.SemaphoreType.DMA
    anywhere = pl.BlockSpec(memory_space=pl.ANY)
    vmem = pl.BlockSpec(memory_space=pltpu.VMEM)
    return pl.pallas_call(
        total_kernel,
        out_shape=(jax.ShapeDtypeStruct(sums.shape, F32), jax.ShapeDtypeStruct(small.shape, F32)),
        in_specs=[anywhere, vmem],
        out_specs=(anywhere, vmem),
        scratch_shapes=[
            pltpu.VMEM((rows, width), F32),
            pltpu.VMEM((rows // 2, width), F32),
            pltpu.VMEM((rows, width), F32),
            pltpu.VMEM((rows // 2, width), BF16),
            pltpu.VMEM((rows // 2, width), BF16),
            pltpu.VMEM((5,) + small.shape, F32),
            pltpu.VMEM((5,) + small.shape, F32),
            dma((3, 5)), dma((3, 5)), dma((3, 5)), dma((3, 5)), dma((5,)), dma((5,)), dma((3,)), dma((3,)),
        ],
        compiler_params=pltpu.CompilerParams(collective_id=1, has_side_effects=True, vmem_limit_bytes=VMEM_LIMIT),
        name="total",
    )(sums, small)


def finish_kernel(up_ref, down_ref, proj_ref, up_out, down_out, proj_out):
    up_out[...] = up_ref[...]
    down_out[...] = down_ref[...].T
    proj_out[...] = proj_ref[...].T


def finish(sums):
    height = sums.shape[0] // 3
    wide = sums.shape[1]
    step = 512
    flat = jax.ShapeDtypeStruct((height, wide), F32)
    tall = jax.ShapeDtypeStruct((wide, height), F32)
    across = pl.BlockSpec((height, step), lambda i: (0, i))
    along = pl.BlockSpec((step, height), lambda i: (i, 0))
    return pl.pallas_call(
        finish_kernel,
        out_shape=(flat, tall, tall),
        grid=(wide // step,),
        in_specs=[pl.BlockSpec((height, step), lambda i, part=part: (part, i)) for part in range(3)],
        out_specs=(across, along, along),
        compiler_params=pltpu.CompilerParams(dimension_semantics=("arbitrary",), vmem_limit_bytes=VMEM_LIMIT),
        name="finish",
    )(sums, sums, sums)


def solution(mesh):
    dev_count = mesh.shape["data"] * mesh.shape["model"]

    def body(teacher_in, student_in, teacher_gain, teacher_up, teacher_down, student_gain, student_up, student_down, student_proj):
        seqs, tokens, t_width = teacher_in.shape
        seq_rows, seq_len, width = student_in.shape
        total = seq_rows * dev_count * seq_len * width
        grad_scale = 2.0 / total
        feature, _, _, rows = teacher_layer(
            teacher_in.reshape(seqs * tokens, t_width), teacher_gain, teacher_up[0], teacher_down[0],
            student_in.reshape(seqs, tokens, width),
        )
        sums, small = student_layer(
            jnp.full((1,), grad_scale, F32), feature, rows.reshape(seqs * tokens, width),
            student_gain, student_up[0], student_down[0], student_proj[0],
        )
        sums, small = total_over_devices(sums, small)
        grad_up, grad_down, grad_proj = finish(sums)
        loss = jnp.sum(small[1]) / total
        return (loss, grad_up[None], grad_down[None], small[None, 0], grad_proj[None])

    return jax.shard_map(
        body,
        mesh=mesh,
        in_specs=(
            P("data", "model", None),
            P(("data", "model"), None, None),
            P(),
            P(None, None, "model"),
            P(None, "model", None),
            P(),
            P(),
            P(),
            P(),
        ),
        out_specs=(P(), P(), P(), P(), P()),
        check_vma=False,
    )
```
